32 devices in a mesh: row: 4 (over x, core), col: 8 (over z, y).
Axes of the slice: x: 2, y: 2, z: 4, core: 2. Of those that a mesh axis runs over, the one named last changes fastest.
Arguments:
- vectors: float32 [32768, 768], P(('row', 'col')), may hold values from -6 to 6
- list_ids: int32 [32768], P(('row', 'col')), may hold values from 0 to 16383, as said below
- pq_codes: int32 [32768, 96], P(('row', 'col')), may hold values from 0 to 255
- fill_counts: int32 [32, 32], P(('row', 'col')), may hold values from 0 to 32, as said below
- centroids: float32 [16384, 768], P(('row', 'col')), may hold values from -6 to 6
- codebook: float32 [96, 8, 256], P('col'), may hold values from -6 to 6
Outputs:
- coded_err: float32 [32768], P(('row', 'col'))
- best_err: float32 [32768], P(('row', 'col'))
The draws below stay inside these ranges and needn't reach their ends.
Inputs may be any that keep to these rules, and one draw needn't show every extreme that they name: `list_ids`: slot s of device p lies in block s // 32, which belongs to owner device s // 32 (devices numbered row-major over row and col); it names a list of that owner, from (s // 32) * 512 to (s // 32 + 1) * 512 - 1. fill_counts[p, d] is the number of live slots at the head of device p's block for owner d; some owner receives 32 live slots from every device.
All inputs are finite; a program needn't handle non-finite values.
Results may differ from the reference program's by a relative error of at most 0.0003.
Values sent between devices are 32-bit elements; how exact they have to be, the bound alone decides.
A program may use at most 256 MiB of HBM per device.

```python
import jax
import jax.numpy as jnp
from jax import lax

D = 768
SUB = 8
M = 96
K = 256
LISTS_DEV = 512
LISTS = 16384
SLOTS_DEV = 1024
CAP = 32
ROWS = 32768
DEVICES = 32


def draw_list_ids(key, part):
    slot_index = jnp.arange(ROWS, dtype=jnp.int32) % SLOTS_DEV
    owner = slot_index // CAP
    local_list = jax.random.randint(jax.random.fold_in(key, 11), (ROWS,), 0, LISTS_DEV, dtype=jnp.int32)
    return owner * LISTS_DEV + local_list


def draw_fill_counts(key, part):
    key_hot = jax.random.fold_in(key, 21)
    key_fill = jax.random.fold_in(key, 22)
    shuffled = jax.random.permutation(key_hot, DEVICES)
    hot_rank = shuffled < max(1, DEVICES // 16)
    base_fill = jax.random.randint(key_fill, (DEVICES, DEVICES), 0, CAP + 1, dtype=jnp.int32)
    return jnp.where(hot_rank[None, :], CAP, base_fill).astype(jnp.int32)


def place_ends(drawn, rng, low, largest):
    spot = [jax.random.randint(jax.random.fold_in(rng, axis), (), 0, length) for axis, length in enumerate(drawn.shape)]
    main_axis = drawn.shape.index(max(drawn.shape))
    neighbour = spot[:main_axis] + [(spot[main_axis] + 1) % drawn.shape[main_axis]] + spot[main_axis + 1:]
    return drawn.at[tuple(spot)].set(low).at[tuple(neighbour)].set(largest)


def block_scale(rng, shape, split, low, top_value):
    loudness = 1.0
    for dim, blocks in split:
        heights = jax.random.uniform(jax.random.fold_in(jax.random.fold_in(rng, 6), dim), (blocks,), jnp.float32, low / len(split), top_value / len(split))
        loudness = loudness * jnp.repeat(jnp.exp(heights), shape[dim] // blocks).reshape((-1,) + (1,) * (len(shape) - 1 - dim))
    return loudness


def centred(key, shape, deviation, bound, cuts=(), kind=jnp.bfloat16):
    result = jax.random.normal(key, shape, jnp.float32) * deviation
    if len(cuts) > 0:
        result = block_scale(key, shape, cuts, -0.22, 0.18) * result
    return jnp.clip(result, min=-bound, max=bound).astype(kind)


def setup_inputs(seed: int = 0) -> dict:
    streams_of = jax.random.split(jax.random.key(seed), 7)
    return {
        "vectors": centred(streams_of[0], (ROWS, D), 1.0, 6.0, ((0, 32),), jnp.float32),
        "list_ids": draw_list_ids(jax.random.fold_in(streams_of[6], 71), 0),
        "pq_codes": place_ends(jax.random.randint(streams_of[2], (ROWS, M), 0, K), jax.random.fold_in(streams_of[2], 1), 0, K - 1).astype(jnp.int32),
        "fill_counts": draw_fill_counts(jax.random.fold_in(streams_of[6], 71), 0),
        "centroids": centred(streams_of[4], (LISTS, D), 1.0, 6.0, ((0, 32),), jnp.float32),
        "codebook": centred(streams_of[5], (M, SUB, K), 1.0, 6.0, ((0, 8),), jnp.float32),
    }


def block_terms(block_vec, block_codes, codebook, code_norms):
    resid_norms = jnp.sum(block_vec * block_vec, axis=2)
    cross_term = jnp.einsum("bms,msk->bmk", block_vec, codebook, precision=lax.Precision.HIGHEST)
    dist_table = resid_norms[:, :, None] - 2.0 * cross_term + code_norms[None, :, :]
    best_sum = jnp.sum(jnp.min(dist_table, axis=2), axis=1)
    code_index = lax.broadcasted_iota(jnp.int32, dist_table.shape, 2)
    coded_sum = jnp.sum(jnp.where(code_index == block_codes[:, :, None], dist_table, 0.0), axis=(1, 2))
    return jnp.stack([coded_sum, best_sum])


def reference(vectors, list_ids, pq_codes, fill_counts, centroids, codebook):
    device_count = fill_counts.shape[0]
    slot_count = vectors.shape[0] // device_count
    capacity = slot_count // device_count
    sub_count = pq_codes.shape[1]
    sub_width = vectors.shape[1] // sub_count
    block_rows = 256
    block_count = slot_count // block_rows
    code_norms = jnp.sum(codebook * codebook, axis=1)

    def one_device(inputs):
        device_vec, device_ids, device_codes = inputs
        residual = device_vec - jnp.take(centroids, device_ids, axis=0)
        shaped = residual.reshape(block_count, block_rows, sub_count, sub_width)
        shaped_codes = device_codes.reshape(block_count, block_rows, sub_count)

        def one_block(pair):
            return block_terms(pair[0], pair[1], codebook, code_norms)

        parts = lax.map(one_block, (shaped, shaped_codes))
        return jnp.transpose(parts, (1, 0, 2)).reshape(2, slot_count)

    results = lax.map(one_device, (vectors.reshape(device_count, slot_count, -1), list_ids.reshape(device_count, slot_count), pq_codes.reshape(device_count, slot_count, sub_count)))
    slot_pos = jnp.arange(capacity, dtype=jnp.int32)
    live_mask = (slot_pos[None, None, :] < fill_counts[:, :, None]).reshape(device_count, slot_count)
    coded_err = jnp.where(live_mask, results[:, 0, :], 0.0).reshape(-1)
    best_err = jnp.where(live_mask, results[:, 1, :], 0.0).reshape(-1)
    return coded_err, best_err
```

```python
import functools

import jax
import jax.numpy as jnp
from jax import lax
from jax.experimental import pallas as pl
from jax.experimental.pallas import tpu as pltpu
from jax.sharding import PartitionSpec as P

F32 = jnp.float32
BF16 = jnp.bfloat16
DEPTH = 64
LANES = 128
PAIRS = 8


def xor(i, s, count):
    out = 0
    bit = 1
    while bit < count:
        out = out + bit * lax.rem(lax.div(i, bit) + lax.div(s, bit), 2)
        bit *= 2
    return out


def split3(x):
    hi = x.astype(BF16).astype(F32)
    rest = x - hi
    mid = rest.astype(BF16).astype(F32)
    return hi, mid, rest - mid


def code_rows(c):
    hi, mid, lo = split3(-2.0 * c)
    norm = jnp.sum(c * c, axis=0, keepdims=True)
    nh, nm, nl = split3(norm)
    line = lax.broadcasted_iota(jnp.int32, c.shape, 0)
    norms = jnp.where(line == 0, nh, jnp.where(line == 1, nm, jnp.where(line == 2, nl, 0.0)))
    return [hi, hi, hi, mid, mid, lo, norms, jnp.zeros_like(c)]


def build_table(cb_ref, w_ref):
    def step(i, carry):
        pieces = code_rows(cb_ref[2 * i]) + code_rows(cb_ref[2 * i + 1])
        w_ref[i] = jnp.concatenate(pieces, axis=0).T.astype(BF16)
        return carry

    lax.fori_loop(0, w_ref.shape[0], step, 0, unroll=2)


def pick(row, idx):
    low = jnp.bitwise_and(idx, LANES - 1)
    got = None
    for part in range(row.shape[1] // LANES):
        piece = jnp.take_along_axis(
            row[:, part * LANES:(part + 1) * LANES], low, axis=1, mode="promise_in_bounds"
        )
        got = piece if got is None else jnp.where(idx >= part * LANES, piece, got)
    return got


def score(rt_ref, codes_ref, base, cb_ref, w_ref):
    sub_count, sub_width, _ = cb_ref.shape
    ones = jnp.ones((sub_width, LANES), F32)
    zeros = jnp.zeros((sub_width, LANES), F32)
    blank = jnp.zeros((DEPTH, LANES), BF16)

    def side(m, code):
        r = rt_ref[pl.ds(pl.multiple_of(m * sub_width, sub_width), sub_width), :]
        hi, mid, lo = split3(r)
        x = jnp.concatenate([hi, mid, lo, hi, mid, hi, ones, zeros], axis=0).astype(BF16)
        diff = r - pick(cb_ref[m], jnp.broadcast_to(code, (sub_width, LANES)))
        return x, r * r, diff * diff

    def step(g, carry):
        coded, norm, best = carry
        codes = codes_ref[pl.ds(pl.multiple_of(g * 2 * PAIRS, 8), 2 * PAIRS), pl.ds(base, LANES)]
        for i in range(PAIRS):
            pair = g * PAIRS + i
            xa, na, da = side(2 * pair, codes[2 * i:2 * i + 1, :])
            xb, nb, db = side(2 * pair + 1, codes[2 * i + 1:2 * i + 2, :])
            x = jnp.concatenate(
                [jnp.concatenate([xa, blank], axis=1), jnp.concatenate([blank, xb], axis=1)], axis=0)
            table = jnp.dot(w_ref[pair], x, preferred_element_type=F32)
            best = best + jnp.min(table, axis=0, keepdims=True)
            norm = norm + (na + nb)
            coded = coded + (da + db)
        return coded, norm, best

    coded, norm, best = lax.fori_loop(
        0, sub_count // (2 * PAIRS), step, (zeros, zeros, jnp.zeros((1, 2 * LANES), F32))
    )
    coded = jnp.sum(coded, axis=0, keepdims=True)
    best = best[:, :LANES] + best[:, LANES:] + jnp.sum(norm, axis=0, keepdims=True)
    return coded, best


def exchange_kernel(row_count, col_count, cb_hbm, v_hbm, codes_hbm, cent_hbm, ids_ref, fill_ref,
                    coded_ref, best_ref,
                    wanted_ref, got_ref, v_ref, cent_ref, codes_ref, book_ref, w_ref, rt_ref, ids_sm,
                    local_sem, ids_send, ids_recv, first_send, second_send, book_recv, rows_send, rows_recv):
    row = lax.axis_index("row")
    col = lax.axis_index("col")
    me = row * col_count + col
    count = row_count * col_count
    sub_local = cb_hbm.shape[0]
    slot_count = v_ref.shape[0]
    capacity = slot_count // count
    lists = cent_ref.shape[0]
    groups = col_count // row_count
    per = LANES // capacity
    spans = col_count // per

    def place(slot):
        return xor(row, lax.div(slot, col_count), row_count), xor(col, lax.rem(slot, col_count), col_count)

    def piece(j):
        return book_ref.at[pl.ds(j * sub_local, sub_local)]

    def block(ref, owner):
        return ref.at[pl.ds(pl.multiple_of(owner * capacity, capacity), capacity)]

    cent_copy = pltpu.make_async_copy(cent_hbm, cent_ref, local_sem.at[0])
    book_copy = pltpu.make_async_copy(cb_hbm, piece(col), local_sem.at[1])
    v_copy = pltpu.make_async_copy(v_hbm, v_ref, local_sem.at[2])
    codes_copy = pltpu.make_async_copy(codes_hbm, codes_ref, local_sem.at[3])
    book_copy.start()
    cent_copy.start()
    v_copy.start()
    codes_copy.start()

    barrier = pltpu.get_barrier_semaphore()

    def greet(slot, carry):
        r, c = place(slot)
        pl.semaphore_signal(barrier, inc=1, device_id=(r, c), device_id_type=pl.DeviceIdType.MESH)
        return carry

    lax.fori_loop(1, count, greet, 0)
    pl.semaphore_wait(barrier, count - 1)

    def ids_copy(slot):
        r, c = place(slot)
        line = lax.div((r * col_count + c) * capacity, LANES)
        return pltpu.make_async_remote_copy(
            src_ref=ids_ref.at[pl.ds(line, 1)], dst_ref=ids_sm.at[pl.ds(me, 1)],
            send_sem=ids_send.at[slot], recv_sem=ids_recv.at[slot],
            device_id=(r, c), device_id_type=pl.DeviceIdType.MESH)

    def ids_arrived(slot):
        r, c = place(slot)
        return pltpu.make_async_remote_copy(
            src_ref=ids_ref.at[pl.ds(0, 1)], dst_ref=ids_sm.at[pl.ds(r * col_count + c, 1)],
            send_sem=ids_send.at[slot], recv_sem=ids_recv.at[slot],
            device_id=(r, c), device_id_type=pl.DeviceIdType.MESH)

    def send_ids(i, carry):
        ids_copy(count - 1 - i).start()
        return carry

    lax.fori_loop(0, count - 1, send_ids, 0)
    own_ids = pltpu.make_async_copy(
        ids_ref.at[pl.ds(lax.div(me * capacity, LANES), 1)], ids_sm.at[pl.ds(me, 1)], local_sem.at[4])
    own_ids.start()

    def first_copy(step):
        return pltpu.make_async_remote_copy(
            src_ref=piece(col), dst_ref=piece(col), send_sem=first_send.at[step], recv_sem=book_recv.at[col],
            device_id=(row, lax.rem(col + step, col_count)), device_id_type=pl.DeviceIdType.MESH)

    def second_copy(group, step):
        j = group * row_count + row
        return pltpu.make_async_remote_copy(
            src_ref=piece(j), dst_ref=piece(j), send_sem=second_send.at[group, step], recv_sem=book_recv.at[j],
            device_id=(lax.rem(row + step, row_count), col), device_id_type=pl.DeviceIdType.MESH)

    def arrived(j):
        return pltpu.make_async_remote_copy(
            src_ref=piece(col), dst_ref=piece(j), send_sem=first_send.at[0], recv_sem=book_recv.at[j],
            device_id=(row, lax.rem(col + 1, col_count)), device_id_type=pl.DeviceIdType.MESH)

    spreads = lax.rem(col, row_count) == row
    book_copy.wait()

    @pl.when(spreads)
    def _():
        for step in range(1, col_count):
            first_copy(step).start()

    offset = lax.rem(me * capacity, LANES)

    def gather(owner, out_ref):
        start = pl.multiple_of(owner * capacity, capacity)

        def some(q, carry):
            for k in range(8):
                j = q * 8 + k
                at = lax.rem(ids_sm[owner, offset + j], lists)
                out_ref[pl.ds(start + j, 1), :] = cent_ref[pl.ds(at, 1), :]
            return carry

        lax.fori_loop(0, capacity // 8, some, 0)

    def rows_copy(slot):
        r, c = place(slot)
        return pltpu.make_async_remote_copy(
            src_ref=block(wanted_ref, r * col_count + c), dst_ref=block(got_ref, me),
            send_sem=rows_send.at[slot], recv_sem=rows_recv.at[slot],
            device_id=(r, c), device_id_type=pl.DeviceIdType.MESH)

    def rows_arrived(slot):
        r, c = place(slot)
        return pltpu.make_async_remote_copy(
            src_ref=block(wanted_ref, me), dst_ref=block(got_ref, r * col_count + c),
            send_sem=rows_send.at[slot], recv_sem=rows_recv.at[slot],
            device_id=(r, c), device_id_type=pl.DeviceIdType.MESH)

    def serve(first, last):
        def one(slot, carry):
            r, c = place(slot)
            ids_arrived(slot).wait_recv()
            gather(r * col_count + c, wanted_ref)

            @pl.when(slot > first)
            def _():
                rows_copy(slot - 1).start()

            return carry

        lax.fori_loop(first, last, one, 0)

    cent_copy.wait()
    half = (row_count // 2) * col_count
    serve(1, half)
    own_ids.wait()
    gather(me, got_ref)
    rows_copy(half - 1).start()

    for group in range(groups):
        @pl.when(group * row_count + row != col)
        def _(group=group):
            arrived(group * row_count + row).wait_recv()
        for step in range(1, row_count):
            @pl.when(group * row_count + row != col)
            def _(group=group, step=step):
                second_copy(group, step).start()

    serve(half, count)
    v_copy.wait()
    codes_copy.wait()
    rows_copy(count - 1).start()

    for group in range(groups):
        for step in range(1, row_count):
            j = group * row_count + lax.rem(row - step + row_count, row_count)

            @pl.when(j != col)
            def _(j=j):
                arrived(j).wait_recv()
    build_table(book_ref, w_ref)

    lane = lax.broadcasted_iota(jnp.int32, (1, LANES), 1)

    def group_step(g, carry):
        a = lax.div(g, 2 * spans) * 2 + lax.rem(g, 2)
        h = lax.rem(lax.div(g, 2), spans)

        def settle(j, inner):
            slot = a * col_count + h * per + j

            @pl.when(slot > 0)
            def _():
                rows_arrived(slot).wait_recv()

            return inner

        lax.fori_loop(0, per, settle, 0)
        first = xor(row, a, row_count) * col_count + xor(lax.div(col, per), h, spans) * per
        base = pl.multiple_of(first * capacity, LANES)
        rt_ref[...] = (v_ref[pl.ds(base, LANES), :] - got_ref[pl.ds(base, LANES), :]).T
        coded, best = score(rt_ref, codes_ref, base, book_ref, w_ref)
        bound = jnp.zeros((1, LANES), jnp.int32)
        for j in range(per):
            bound = jnp.where(lane >= j * capacity, fill_ref[0, first + j] + j * capacity, bound)
        live = lane < bound
        coded_ref[:, pl.ds(base, LANES)] = jnp.where(live, coded, 0.0)
        best_ref[:, pl.ds(base, LANES)] = jnp.where(live, best, 0.0)
        return carry

    lax.fori_loop(0, row_count * spans, group_step, 0)

    @pl.when(spreads)
    def _():
        for step in range(1, col_count):
            first_copy(step).wait_send()

    for group in range(groups):
        @pl.when(group * row_count + row != col)
        def _(group=group):
            for step in range(1, row_count):
                second_copy(group, step).wait_send()

    def drain(slot, carry):
        ids_copy(slot).wait_send()
        rows_copy(slot).wait_send()
        return carry

    lax.fori_loop(1, count, drain, 0)


def local(vectors, list_ids, pq_codes, fill_counts, centroids, codebook):
    row_count = lax.axis_size("row")
    col_count = lax.axis_size("col")
    count = row_count * col_count
    slot_count, feature_width = vectors.shape
    sub_total = pq_codes.shape[1]
    sub_width, code_count = codebook.shape[1:]
    vmem = pl.BlockSpec(memory_space=pltpu.VMEM)
    smem = pl.BlockSpec(memory_space=pltpu.SMEM)
    hbm = pl.BlockSpec(memory_space=pl.ANY)
    coded, best = pl.pallas_call(
        functools.partial(exchange_kernel, row_count, col_count),
        out_shape=[jax.ShapeDtypeStruct((1, slot_count), F32)] * 2,
        in_specs=[hbm] * 4 + [vmem, smem],
        out_specs=[vmem] * 2,
        scratch_shapes=[
            pltpu.VMEM((slot_count, feature_width), F32),
            pltpu.VMEM((slot_count, feature_width), F32),
            pltpu.VMEM((slot_count, feature_width), F32),
            pltpu.VMEM(centroids.shape, F32),
            pltpu.VMEM((sub_total, slot_count), jnp.int32),
            pltpu.VMEM((sub_total, sub_width, code_count), F32),
            pltpu.VMEM((sub_total // 2, code_count, 2 * DEPTH), BF16),
            pltpu.VMEM((feature_width, LANES), F32),
            pltpu.SMEM((count, LANES), jnp.int32),
            pltpu.SemaphoreType.DMA((5,)),
            pltpu.SemaphoreType.DMA((count,)),
            pltpu.SemaphoreType.DMA((count,)),
            pltpu.SemaphoreType.DMA((col_count,)),
            pltpu.SemaphoreType.DMA((col_count // row_count, row_count)),
            pltpu.SemaphoreType.DMA((col_count,)),
            pltpu.SemaphoreType.DMA((count,)),
            pltpu.SemaphoreType.DMA((count,)),
        ],
        compiler_params=pltpu.CompilerParams(
            collective_id=0, has_side_effects=True, vmem_limit_bytes=56 * 2**20),
        name="exchange_score",
    )(codebook, vectors, pq_codes.T, centroids, list_ids.reshape(slot_count // LANES, LANES), fill_counts)
    return coded.reshape(slot_count), best.reshape(slot_count)


def solution(mesh):
    in_specs = (
        P(("row", "col"), None),
        P(("row", "col")),
        P(("row", "col"), None),
        P(("row", "col"), None),
        P(("row", "col"), None),
        P("col", None, None),
    )
    out_specs = (P(("row", "col")), P(("row", "col")))
    return jax.shard_map(local, mesh=mesh, in_specs=in_specs, out_specs=out_specs, check_vma=False)
```

```python
import functools

import jax
import jax.numpy as jnp
from jax import lax
from jax.experimental import pallas as pl
from jax.experimental.pallas import tpu as pltpu
from jax.sharding import PartitionSpec as P

F32 = jnp.float32
BF16 = jnp.bfloat16
DEPTH = 64
LANES = 128
PAIRS = 8


def xor(i, s, count):
    out = 0
    bit = 1
    while bit < count:
        out = out + bit * lax.rem(lax.div(i, bit) + lax.div(s, bit), 2)
        bit *= 2
    return out


def split3(x):
    hi = x.astype(BF16).astype(F32)
    rest = x - hi
    mid = rest.astype(BF16).astype(F32)
    return hi, mid, rest - mid


def code_rows(c):
    hi, mid, lo = split3(-2.0 * c)
    norm = jnp.sum(c * c, axis=0, keepdims=True)
    nh, nm, nl = split3(norm)
    line = lax.broadcasted_iota(jnp.int32, c.shape, 0)
    norms = jnp.where(line == 0, nh, jnp.where(line == 1, nm, jnp.where(line == 2, nl, 0.0)))
    return [hi, hi, hi, mid, mid, lo, norms, jnp.zeros_like(c)]


def build_table(cb_ref, w_ref):
    def step(i, carry):
        pieces = code_rows(cb_ref[2 * i]) + code_rows(cb_ref[2 * i + 1])
        w_ref[i] = jnp.concatenate(pieces, axis=0).T.astype(BF16)
        return carry

    lax.fori_loop(0, w_ref.shape[0], step, 0, unroll=2)


def pick(row, idx):
    low = jnp.bitwise_and(idx, LANES - 1)
    got = None
    for part in range(row.shape[1] // LANES):
        piece = jnp.take_along_axis(
            row[:, part * LANES:(part + 1) * LANES], low, axis=1, mode="promise_in_bounds"
        )
        got = piece if got is None else jnp.where(idx >= part * LANES, piece, got)
    return got


def score_step(g, carry, rt_ref, codes_ref, base, cb_ref, w_ref):
    sub_width = cb_ref.shape[1]
    ones = jnp.ones((sub_width, LANES), F32)
    zeros = jnp.zeros((sub_width, LANES), F32)
    blank = jnp.zeros((DEPTH, LANES), BF16)

    def side(m, code):
        r = rt_ref[pl.ds(pl.multiple_of(m * sub_width, sub_width), sub_width), :]
        hi, mid, lo = split3(r)
        x = jnp.concatenate([hi, mid, lo, hi, mid, hi, ones, zeros], axis=0).astype(BF16)
        diff = r - pick(cb_ref[m], jnp.broadcast_to(code, (sub_width, LANES)))
        return x, r * r, diff * diff

    coded, norm, best = carry
    codes = codes_ref[pl.ds(pl.multiple_of(g * 2 * PAIRS, 8), 2 * PAIRS), pl.ds(base, LANES)]
    for i in range(PAIRS):
        pair = g * PAIRS + i
        xa, na, da = side(2 * pair, codes[2 * i:2 * i + 1, :])
        xb, nb, db = side(2 * pair + 1, codes[2 * i + 1:2 * i + 2, :])
        x = jnp.concatenate(
            [jnp.concatenate([xa, blank], axis=1), jnp.concatenate([blank, xb], axis=1)], axis=0)
        table = jnp.dot(w_ref[pair], x, preferred_element_type=F32)
        best = best + jnp.min(table, axis=0, keepdims=True)
        norm = norm + (na + nb)
        coded = coded + (da + db)
    return coded, norm, best


def score_start(sub_width):
    zeros = jnp.zeros((sub_width, LANES), F32)
    return zeros, zeros, jnp.zeros((1, 2 * LANES), F32)


def score_end(carry):
    coded, norm, best = carry
    coded = jnp.sum(coded, axis=0, keepdims=True)
    return coded, best[:, :LANES] + best[:, LANES:] + jnp.sum(norm, axis=0, keepdims=True)


def exchange_kernel(row_count, col_count, cb_hbm, v_hbm, codes_hbm, cent_hbm, ids_ref, fill_ref,
                    coded_ref, best_ref, live_ref,
                    wanted_ref, got_ref, v_ref, cent_ref, codes_ref, book_ref, w_ref, rt_ref, ids_sm,
                    local_sem, ids_send, ids_recv, first_send, mirror_send, second_send, book_recv,
                    rows_send, rows_recv, last_send, last_recv):
    row = lax.axis_index("row")
    col = lax.axis_index("col")
    me = row * col_count + col
    count = row_count * col_count
    sub_local = cb_hbm.shape[0]
    slot_count = v_ref.shape[0]
    capacity = slot_count // count
    lists = cent_ref.shape[0]
    groups = col_count // row_count
    per = LANES // capacity
    spans = col_count // per
    top = col_count // 2
    mirror = xor(col, top, col_count)
    steps = v_ref.shape[1] // LANES
    last = count - per

    def place(slot):
        return xor(row, lax.div(slot, col_count), row_count), xor(col, lax.rem(slot, col_count), col_count)

    def piece(j):
        return book_ref.at[pl.ds(j * sub_local, sub_local)]

    def block(ref, owner):
        return ref.at[pl.ds(pl.multiple_of(owner * capacity, capacity), capacity)]

    cent_copy = pltpu.make_async_copy(cent_hbm, cent_ref, local_sem.at[0])
    book_copy = pltpu.make_async_copy(cb_hbm, piece(col), local_sem.at[1])
    v_copy = pltpu.make_async_copy(v_hbm, v_ref, local_sem.at[2])
    codes_copy = pltpu.make_async_copy(codes_hbm, codes_ref, local_sem.at[3])
    book_copy.start()
    cent_copy.start()
    v_copy.start()
    codes_copy.start()

    barrier = pltpu.get_barrier_semaphore()

    def greet(slot, carry):
        r, c = place(slot)
        pl.semaphore_signal(barrier, inc=1, device_id=(r, c), device_id_type=pl.DeviceIdType.MESH)
        return carry

    lax.fori_loop(1, count, greet, 0)
    pl.semaphore_wait(barrier, count - 1)

    def ids_copy(slot):
        r, c = place(slot)
        line = lax.div((r * col_count + c) * capacity, LANES)
        return pltpu.make_async_remote_copy(
            src_ref=ids_ref.at[pl.ds(line, 1)], dst_ref=ids_sm.at[pl.ds(me, 1)],
            send_sem=ids_send.at[slot], recv_sem=ids_recv.at[slot],
            device_id=(r, c), device_id_type=pl.DeviceIdType.MESH)

    def ids_arrived(slot):
        r, c = place(slot)
        return pltpu.make_async_remote_copy(
            src_ref=ids_ref.at[pl.ds(0, 1)], dst_ref=ids_sm.at[pl.ds(r * col_count + c, 1)],
            send_sem=ids_send.at[slot], recv_sem=ids_recv.at[slot],
            device_id=(r, c), device_id_type=pl.DeviceIdType.MESH)

    def send_ids(i, carry):
        ids_copy(count - 1 - i).start()
        return carry

    lax.fori_loop(0, count - 1, send_ids, 0)
    own_ids = pltpu.make_async_copy(
        ids_ref.at[pl.ds(lax.div(me * capacity, LANES), 1)], ids_sm.at[pl.ds(me, 1)], local_sem.at[4])
    own_ids.start()

    def book_copy_to(source, target, sem):
        return pltpu.make_async_remote_copy(
            src_ref=piece(source), dst_ref=piece(source), send_sem=sem, recv_sem=book_recv.at[source],
            device_id=(row, target), device_id_type=pl.DeviceIdType.MESH)

    def second_copy(group, step):
        j = group * row_count + row
        return pltpu.make_async_remote_copy(
            src_ref=piece(j), dst_ref=piece(j), send_sem=second_send.at[group, step], recv_sem=book_recv.at[j],
            device_id=(lax.rem(row + step, row_count), col), device_id_type=pl.DeviceIdType.MESH)

    def arrived(j):
        return book_copy_to(j, mirror, first_send.at[0])

    def spread(source, sems):
        return [book_copy_to(source, xor(col, b, col_count), sems.at[b]) for b in range(1, top)]

    spreads = lax.rem(col, row_count) == row
    book_copy.wait()

    @pl.when(spreads)
    def _():
        book_copy_to(col, mirror, first_send.at[0]).start()
        for copy in spread(col, first_send):
            copy.start()

    offset = lax.rem(me * capacity, LANES)

    def gather(owner, out_ref):
        start = pl.multiple_of(owner * capacity, capacity)

        def some(q, carry):
            for k in range(8):
                j = q * 8 + k
                at = lax.rem(ids_sm[owner, offset + j], lists)
                out_ref[pl.ds(start + j, 1), :] = cent_ref[pl.ds(at, 1), :]
            return carry

        lax.fori_loop(0, capacity // 8, some, 0)

    def rows_copy(slot):
        r, c = place(slot)
        return pltpu.make_async_remote_copy(
            src_ref=block(wanted_ref, r * col_count + c), dst_ref=block(got_ref, me),
            send_sem=rows_send.at[slot], recv_sem=rows_recv.at[slot],
            device_id=(r, c), device_id_type=pl.DeviceIdType.MESH)

    def rows_arrived(slot):
        r, c = place(slot)
        return pltpu.make_async_remote_copy(
            src_ref=block(wanted_ref, me), dst_ref=block(got_ref, r * col_count + c),
            send_sem=rows_send.at[slot], recv_sem=rows_recv.at[slot],
            device_id=(r, c), device_id_type=pl.DeviceIdType.MESH)

    def last_copy(j, f):
        r, c = place(last + j)
        part = pl.ds(pl.multiple_of(f * LANES, LANES), LANES)
        return pltpu.make_async_remote_copy(
            src_ref=block(wanted_ref, r * col_count + c).at[:, part], dst_ref=block(got_ref, me).at[:, part],
            send_sem=last_send.at[f, j], recv_sem=last_recv.at[f, j],
            device_id=(r, c), device_id_type=pl.DeviceIdType.MESH)

    def last_arrived(j, f):
        r, c = place(last + j)
        part = pl.ds(pl.multiple_of(f * LANES, LANES), LANES)
        return pltpu.make_async_remote_copy(
            src_ref=block(wanted_ref, me).at[:, part], dst_ref=block(got_ref, r * col_count + c).at[:, part],
            send_sem=last_send.at[f, j], recv_sem=last_recv.at[f, j],
            device_id=(r, c), device_id_type=pl.DeviceIdType.MESH)

    def serve(first, end):
        def one(slot, carry):
            r, c = place(slot)
            ids_arrived(slot).wait_recv()
            gather(r * col_count + c, wanted_ref)

            @pl.when(slot > first)
            def _():
                @pl.when(slot <= last)
                def _():
                    rows_copy(slot - 1).start()

            return carry

        lax.fori_loop(first, end, one, 0)

    cent_copy.wait()
    half = (row_count // 2) * col_count
    serve(1, half)
    own_ids.wait()
    gather(me, got_ref)
    rows_copy(half - 1).start()

    @pl.when(spreads)
    def _():
        arrived(mirror).wait_recv()
        for copy in spread(mirror, mirror_send):
            copy.start()

    for group in range(groups):
        j = group * row_count + row

        @pl.when((j - col) * (j - mirror) != 0)
        def _(j=j):
            arrived(j).wait_recv()

        @pl.when(j != col)
        def _(group=group):
            for step in range(1, row_count):
                second_copy(group, step).start()

    serve(half, count)
    v_copy.wait()
    codes_copy.wait()

    def send_last(i, carry):
        last_copy(lax.rem(i, per), lax.div(i, per)).start()
        return carry

    lax.fori_loop(0, per * steps, send_last, 0)

    for group in range(groups):
        for step in range(1, row_count):
            j = group * row_count + lax.rem(row - step + row_count, row_count)

            @pl.when(j != col)
            def _(j=j):
                arrived(j).wait_recv()
    build_table(book_ref, w_ref)

    lane = lax.broadcasted_iota(jnp.int32, (1, LANES), 1)
    sub_width = book_ref.shape[1]

    def group_at(g):
        a = lax.div(g, 2 * spans) * 2 + lax.rem(g, 2)
        h = lax.rem(lax.div(g, 2), spans)
        first = xor(row, a, row_count) * col_count + xor(lax.div(col, per), h, spans) * per
        return a * col_count + h * per, first, pl.multiple_of(first * capacity, LANES)

    def finish(carry, first, base):
        coded, best = score_end(carry)
        bound = jnp.zeros((1, LANES), jnp.int32)
        for j in range(per):
            bound = jnp.where(lane >= j * capacity, fill_ref[0, first + j] + j * capacity, bound)
        coded_ref[:, pl.ds(base, LANES)] = coded
        best_ref[:, pl.ds(base, LANES)] = best
        live_ref[:, pl.ds(base, LANES)] = jnp.where(lane < bound, 1, 0)

    def group_step(g, carry):
        slot, first, base = group_at(g)

        def settle(j, inner):
            @pl.when(slot + j > 0)
            def _():
                rows_arrived(slot + j).wait_recv()

            return inner

        lax.fori_loop(0, per, settle, 0)
        rt_ref[...] = (v_ref[pl.ds(base, LANES), :] - got_ref[pl.ds(base, LANES), :]).T

        def step(f, inner):
            return score_step(f, inner, rt_ref, codes_ref, base, book_ref, w_ref)

        finish(lax.fori_loop(0, steps, step, score_start(sub_width)), first, base)
        return carry

    lax.fori_loop(0, row_count * spans - 1, group_step, 0)

    _, first, base = group_at(row_count * spans - 1)

    def last_step(f, carry):
        for j in range(per):
            last_arrived(j, f).wait_recv()
        part = pl.ds(pl.multiple_of(f * LANES, LANES), LANES)
        rt_ref[part, :] = (v_ref[pl.ds(base, LANES), part] - got_ref[pl.ds(base, LANES), part]).T
        return score_step(f, carry, rt_ref, codes_ref, base, book_ref, w_ref)

    finish(lax.fori_loop(0, steps, last_step, score_start(sub_width)), first, base)

    @pl.when(spreads)
    def _():
        book_copy_to(col, mirror, first_send.at[0]).wait_send()
        for copy in spread(col, first_send) + spread(mirror, mirror_send):
            copy.wait_send()

    for group in range(groups):
        @pl.when(group * row_count + row != col)
        def _(group=group):
            for step in range(1, row_count):
                second_copy(group, step).wait_send()

    def drain_ids(slot, carry):
        ids_copy(slot).wait_send()
        return carry

    def drain_rows(slot, carry):
        rows_copy(slot).wait_send()
        return carry

    def drain_last(i, carry):
        last_copy(lax.rem(i, per), lax.div(i, per)).wait_send()
        return carry

    lax.fori_loop(1, count, drain_ids, 0)
    lax.fori_loop(1, last, drain_rows, 0)
    lax.fori_loop(0, per * steps, drain_last, 0)


def local(vectors, list_ids, pq_codes, fill_counts, centroids, codebook):
    row_count = lax.axis_size("row")
    col_count = lax.axis_size("col")
    count = row_count * col_count
    slot_count, feature_width = vectors.shape
    sub_total = pq_codes.shape[1]
    sub_width, code_count = codebook.shape[1:]
    per = LANES * count // slot_count
    vmem = pl.BlockSpec(memory_space=pltpu.VMEM)
    smem = pl.BlockSpec(memory_space=pltpu.SMEM)
    hbm = pl.BlockSpec(memory_space=pl.ANY)
    coded, best, live = pl.pallas_call(
        functools.partial(exchange_kernel, row_count, col_count),
        out_shape=[jax.ShapeDtypeStruct((1, slot_count), kind) for kind in (F32, F32, jnp.int32)],
        in_specs=[hbm] * 4 + [vmem, smem],
        out_specs=[vmem] * 3,
        scratch_shapes=[
            pltpu.VMEM((slot_count, feature_width), F32),
            pltpu.VMEM((slot_count, feature_width), F32),
            pltpu.VMEM((slot_count, feature_width), F32),
            pltpu.VMEM(centroids.shape, F32),
            pltpu.VMEM((sub_total, slot_count), jnp.int32),
            pltpu.VMEM((sub_total, sub_width, code_count), F32),
            pltpu.VMEM((sub_total // 2, code_count, 2 * DEPTH), BF16),
            pltpu.VMEM((feature_width, LANES), F32),
            pltpu.SMEM((count, LANES), jnp.int32),
            pltpu.SemaphoreType.DMA((5,)),
            pltpu.SemaphoreType.DMA((count,)),
            pltpu.SemaphoreType.DMA((count,)),
            pltpu.SemaphoreType.DMA((col_count // 2,)),
            pltpu.SemaphoreType.DMA((col_count // 2,)),
            pltpu.SemaphoreType.DMA((col_count // row_count, row_count)),
            pltpu.SemaphoreType.DMA((col_count,)),
            pltpu.SemaphoreType.DMA((count,)),
            pltpu.SemaphoreType.DMA((count,)),
            pltpu.SemaphoreType.DMA((feature_width // LANES, per)),
            pltpu.SemaphoreType.DMA((feature_width // LANES, per)),
        ],
        compiler_params=pltpu.CompilerParams(
            collective_id=0, has_side_effects=True, vmem_limit_bytes=56 * 2**20),
        name="exchange_score",
    )(codebook, vectors, pq_codes.T, centroids, list_ids.reshape(slot_count // LANES, LANES), fill_counts)
    alive = live.reshape(slot_count) > 0
    return jnp.where(alive, coded.reshape(slot_count), 0.0), jnp.where(alive, best.reshape(slot_count), 0.0)


def solution(mesh):
    in_specs = (
        P(("row", "col"), None),
        P(("row", "col")),
        P(("row", "col"), None),
        P(("row", "col"), None),
        P(("row", "col"), None),
        P("col", None, None),
    )
    out_specs = (P(("row", "col")), P(("row", "col")))
    return jax.shard_map(local, mesh=mesh, in_specs=in_specs, out_specs=out_specs, check_vma=False)
```

```python
import functools

import jax
import jax.numpy as jnp
from jax import lax
from jax.experimental import pallas as pl
from jax.experimental.pallas import tpu as pltpu
from jax.sharding import PartitionSpec as P

F32 = jnp.float32
BF16 = jnp.bfloat16
DEPTH = 64
LANES = 128
PAIRS = 8
SLICES = 2


def xor(i, s, count):
    out = 0
    bit = 1
    while bit < count:
        out = out + bit * lax.rem(lax.div(i, bit) + lax.div(s, bit), 2)
        bit *= 2
    return out


def split3(x):
    hi = x.astype(BF16).astype(F32)
    rest = x - hi
    mid = rest.astype(BF16).astype(F32)
    return hi, mid, rest - mid


def code_rows(c):
    hi, mid, lo = split3(-2.0 * c)
    norm = jnp.sum(c * c, axis=0, keepdims=True)
    nh, nm, nl = split3(norm)
    line = lax.broadcasted_iota(jnp.int32, c.shape, 0)
    norms = jnp.where(line == 0, nh, jnp.where(line == 1, nm, jnp.where(line == 2, nl, 0.0)))
    return [hi, hi, hi, mid, mid, lo, norms, jnp.zeros_like(c)]


def build_table(cb_ref, w_ref):
    def step(i, carry):
        pieces = code_rows(cb_ref[2 * i]) + code_rows(cb_ref[2 * i + 1])
        w_ref[i] = jnp.concatenate(pieces, axis=0).T.astype(BF16)
        return carry

    lax.fori_loop(0, w_ref.shape[0], step, 0, unroll=2)


def pick(row, idx):
    low = jnp.bitwise_and(idx, LANES - 1)
    got = None
    for part in range(row.shape[1] // LANES):
        piece = jnp.take_along_axis(
            row[:, part * LANES:(part + 1) * LANES], low, axis=1, mode="promise_in_bounds"
        )
        got = piece if got is None else jnp.where(idx >= part * LANES, piece, got)
    return got


def score_step(g, carry, rt_ref, codes_ref, base, cb_ref, w_ref):
    sub_width = cb_ref.shape[1]
    ones = jnp.ones((sub_width, LANES), F32)
    zeros = jnp.zeros((sub_width, LANES), F32)
    blank = jnp.zeros((DEPTH, LANES), BF16)

    def side(m, code):
        r = rt_ref[pl.ds(pl.multiple_of(m * sub_width, sub_width), sub_width), :]
        hi, mid, lo = split3(r)
        x = jnp.concatenate([hi, mid, lo, hi, mid, hi, ones, zeros], axis=0).astype(BF16)
        diff = r - pick(cb_ref[m], jnp.broadcast_to(code, (sub_width, LANES)))
        return x, r * r, diff * diff

    coded, norm, best = carry
    codes = codes_ref[pl.ds(pl.multiple_of(g * 2 * PAIRS, 8), 2 * PAIRS), pl.ds(base, LANES)]
    for i in range(PAIRS):
        pair = g * PAIRS + i
        xa, na, da = side(2 * pair, codes[2 * i:2 * i + 1, :])
        xb, nb, db = side(2 * pair + 1, codes[2 * i + 1:2 * i + 2, :])
        x = jnp.concatenate(
            [jnp.concatenate([xa, blank], axis=1), jnp.concatenate([blank, xb], axis=1)], axis=0)
        table = jnp.dot(w_ref[pair], x, preferred_element_type=F32)
        best = best + jnp.min(table, axis=0, keepdims=True)
        norm = norm + (na + nb)
        coded = coded + (da + db)
    return coded, norm, best


def score_start(sub_width):
    zeros = jnp.zeros((sub_width, LANES), F32)
    return zeros, zeros, jnp.zeros((1, 2 * LANES), F32)


def score_end(carry):
    coded, norm, best = carry
    coded = jnp.sum(coded, axis=0, keepdims=True)
    return coded, best[:, :LANES] + best[:, LANES:] + jnp.sum(norm, axis=0, keepdims=True)


def exchange_kernel(row_count, col_count, cb_hbm, v_hbm, codes_hbm, cent_hbm, ids_ref, fill_ref,
                    coded_ref, best_ref, live_ref,
                    wanted_ref, got_ref, v_ref, cent_ref, codes_ref, book_ref, w_ref, rt_ref, ids_sm,
                    local_sem, ids_send, ids_recv, first_send, mirror_send, second_send, book_recv,
                    rows_send, rows_recv, last_send, last_recv):
    row = lax.axis_index("row")
    col = lax.axis_index("col")
    me = row * col_count + col
    count = row_count * col_count
    sub_local = cb_hbm.shape[0]
    slot_count = v_ref.shape[0]
    capacity = slot_count // count
    lists = cent_ref.shape[0]
    groups = col_count // row_count
    per = LANES // capacity
    spans = col_count // per
    top = col_count // 2
    mirror = xor(col, top, col_count)
    steps = v_ref.shape[1] // LANES
    last = count - per
    slice_width = v_ref.shape[1] // SLICES
    slice_steps = steps // SLICES

    def place(slot):
        return xor(row, lax.div(slot, col_count), row_count), xor(col, lax.rem(slot, col_count), col_count)

    def piece(j):
        return book_ref.at[pl.ds(j * sub_local, sub_local)]

    def block(ref, owner):
        return ref.at[pl.ds(pl.multiple_of(owner * capacity, capacity), capacity)]

    cent_copy = pltpu.make_async_copy(cent_hbm, cent_ref, local_sem.at[0])
    book_copy = pltpu.make_async_copy(cb_hbm, piece(col), local_sem.at[1])
    v_copy = pltpu.make_async_copy(v_hbm, v_ref, local_sem.at[2])
    codes_copy = pltpu.make_async_copy(codes_hbm, codes_ref, local_sem.at[3])
    book_copy.start()
    cent_copy.start()
    v_copy.start()
    codes_copy.start()

    barrier = pltpu.get_barrier_semaphore()

    def greet(slot, carry):
        r, c = place(slot)
        pl.semaphore_signal(barrier, inc=1, device_id=(r, c), device_id_type=pl.DeviceIdType.MESH)
        return carry

    lax.fori_loop(1, count, greet, 0)
    pl.semaphore_wait(barrier, count - 1)

    def ids_copy(slot):
        r, c = place(slot)
        line = lax.div((r * col_count + c) * capacity, LANES)
        return pltpu.make_async_remote_copy(
            src_ref=ids_ref.at[pl.ds(line, 1)], dst_ref=ids_sm.at[pl.ds(me, 1)],
            send_sem=ids_send.at[slot], recv_sem=ids_recv.at[slot],
            device_id=(r, c), device_id_type=pl.DeviceIdType.MESH)

    def ids_arrived(slot):
        r, c = place(slot)
        return pltpu.make_async_remote_copy(
            src_ref=ids_ref.at[pl.ds(0, 1)], dst_ref=ids_sm.at[pl.ds(r * col_count + c, 1)],
            send_sem=ids_send.at[slot], recv_sem=ids_recv.at[slot],
            device_id=(r, c), device_id_type=pl.DeviceIdType.MESH)

    def send_ids(i, carry):
        ids_copy(count - 1 - i).start()
        return carry

    lax.fori_loop(0, count - 1, send_ids, 0)
    own_ids = pltpu.make_async_copy(
        ids_ref.at[pl.ds(lax.div(me * capacity, LANES), 1)], ids_sm.at[pl.ds(me, 1)], local_sem.at[4])
    own_ids.start()

    def book_copy_to(source, target, sem):
        return pltpu.make_async_remote_copy(
            src_ref=piece(source), dst_ref=piece(source), send_sem=sem, recv_sem=book_recv.at[source],
            device_id=(row, target), device_id_type=pl.DeviceIdType.MESH)

    def second_copy(group, step):
        j = group * row_count + row
        return pltpu.make_async_remote_copy(
            src_ref=piece(j), dst_ref=piece(j), send_sem=second_send.at[group, step], recv_sem=book_recv.at[j],
            device_id=(lax.rem(row + step, row_count), col), device_id_type=pl.DeviceIdType.MESH)

    def arrived(j):
        return book_copy_to(j, mirror, first_send.at[0])

    def spread(source, sems):
        return [book_copy_to(source, xor(col, b, col_count), sems.at[b]) for b in range(1, top)]

    spreads = lax.rem(col, row_count) == row
    book_copy.wait()

    @pl.when(spreads)
    def _():
        book_copy_to(col, mirror, first_send.at[0]).start()
        for copy in spread(col, first_send):
            copy.start()

    offset = lax.rem(me * capacity, LANES)

    def gather(owner, out_ref):
        start = pl.multiple_of(owner * capacity, capacity)

        def some(q, carry):
            for k in range(8):
                j = q * 8 + k
                at = lax.rem(ids_sm[owner, offset + j], lists)
                out_ref[pl.ds(start + j, 1), :] = cent_ref[pl.ds(at, 1), :]
            return carry

        lax.fori_loop(0, capacity // 8, some, 0)

    def rows_copy(slot):
        r, c = place(slot)
        return pltpu.make_async_remote_copy(
            src_ref=block(wanted_ref, r * col_count + c), dst_ref=block(got_ref, me),
            send_sem=rows_send.at[slot], recv_sem=rows_recv.at[slot],
            device_id=(r, c), device_id_type=pl.DeviceIdType.MESH)

    def rows_arrived(slot):
        r, c = place(slot)
        return pltpu.make_async_remote_copy(
            src_ref=block(wanted_ref, me), dst_ref=block(got_ref, r * col_count + c),
            send_sem=rows_send.at[slot], recv_sem=rows_recv.at[slot],
            device_id=(r, c), device_id_type=pl.DeviceIdType.MESH)

    def last_copy(j, f):
        r, c = place(last + j)
        part = pl.ds(pl.multiple_of(f * slice_width, LANES), slice_width)
        return pltpu.make_async_remote_copy(
            src_ref=block(wanted_ref, r * col_count + c).at[:, part], dst_ref=block(got_ref, me).at[:, part],
            send_sem=last_send.at[f, j], recv_sem=last_recv.at[f, j],
            device_id=(r, c), device_id_type=pl.DeviceIdType.MESH)

    def last_arrived(j, f):
        r, c = place(last + j)
        part = pl.ds(pl.multiple_of(f * slice_width, LANES), slice_width)
        return pltpu.make_async_remote_copy(
            src_ref=block(wanted_ref, me).at[:, part], dst_ref=block(got_ref, r * col_count + c).at[:, part],
            send_sem=last_send.at[f, j], recv_sem=last_recv.at[f, j],
            device_id=(r, c), device_id_type=pl.DeviceIdType.MESH)

    def serve(first, end):
        def one(slot, carry):
            r, c = place(slot)
            ids_arrived(slot).wait_recv()
            gather(r * col_count + c, wanted_ref)

            @pl.when(slot > first)
            def _():
                @pl.when(slot <= last)
                def _():
                    rows_copy(slot - 1).start()

            return carry

        lax.fori_loop(first, end, one, 0)

    cent_copy.wait()
    half = (row_count // 2) * col_count
    serve(top, col_count)
    own_ids.wait()
    gather(me, got_ref)
    rows_copy(col_count - 1).start()

    @pl.when(spreads)
    def _():
        arrived(mirror).wait_recv()
        for copy in spread(mirror, mirror_send):
            copy.start()

    serve(1, top)
    serve(col_count, half)
    rows_copy(top - 1).start()
    rows_copy(half - 1).start()

    for group in range(groups):
        j = group * row_count + row

        @pl.when((j - col) * (j - mirror) != 0)
        def _(j=j):
            arrived(j).wait_recv()

        @pl.when(j != col)
        def _(group=group):
            for step in range(1, row_count):
                second_copy(group, step).start()

    serve(half, count)
    v_copy.wait()
    codes_copy.wait()

    def send_last(i, carry):
        last_copy(lax.rem(i, per), lax.div(i, per)).start()
        return carry

    lax.fori_loop(0, per * SLICES, send_last, 0)

    for group in range(groups):
        for step in range(1, row_count):
            j = group * row_count + lax.rem(row - step + row_count, row_count)

            @pl.when(j != col)
            def _(j=j):
                arrived(j).wait_recv()
    build_table(book_ref, w_ref)

    lane = lax.broadcasted_iota(jnp.int32, (1, LANES), 1)
    sub_width = book_ref.shape[1]

    def group_at(g):
        a = lax.div(g, 2 * spans) * 2 + lax.rem(g, 2)
        h = lax.rem(lax.div(g, 2), spans)
        first = xor(row, a, row_count) * col_count + xor(lax.div(col, per), h, spans) * per
        return a * col_count + h * per, first, pl.multiple_of(first * capacity, LANES)

    def finish(carry, first, base):
        coded, best = score_end(carry)
        bound = jnp.zeros((1, LANES), jnp.int32)
        for j in range(per):
            bound = jnp.where(lane >= j * capacity, fill_ref[0, first + j] + j * capacity, bound)
        coded_ref[:, pl.ds(base, LANES)] = coded
        best_ref[:, pl.ds(base, LANES)] = best
        live_ref[:, pl.ds(base, LANES)] = jnp.where(lane < bound, 1, 0)

    def group_step(g, carry):
        slot, first, base = group_at(g)

        def settle(j, inner):
            @pl.when(slot + j > 0)
            def _():
                rows_arrived(slot + j).wait_recv()

            return inner

        lax.fori_loop(0, per, settle, 0)
        rt_ref[...] = (v_ref[pl.ds(base, LANES), :] - got_ref[pl.ds(base, LANES), :]).T

        def step(f, inner):
            return score_step(f, inner, rt_ref, codes_ref, base, book_ref, w_ref)

        finish(lax.fori_loop(0, steps, step, score_start(sub_width)), first, base)
        return carry

    lax.fori_loop(0, row_count * spans - 1, group_step, 0)

    _, first, base = group_at(row_count * spans - 1)

    carry = score_start(sub_width)
    for f in range(SLICES):
        for j in range(per):
            last_arrived(j, f).wait_recv()
        part = pl.ds(f * slice_width, slice_width)
        rt_ref[part, :] = (v_ref[pl.ds(base, LANES), part] - got_ref[pl.ds(base, LANES), part]).T

        def last_step(g, inner):
            return score_step(g, inner, rt_ref, codes_ref, base, book_ref, w_ref)

        carry = lax.fori_loop(f * slice_steps, (f + 1) * slice_steps, last_step, carry)
    finish(carry, first, base)

    @pl.when(spreads)
    def _():
        book_copy_to(col, mirror, first_send.at[0]).wait_send()
        for copy in spread(col, first_send) + spread(mirror, mirror_send):
            copy.wait_send()

    for group in range(groups):
        @pl.when(group * row_count + row != col)
        def _(group=group):
            for step in range(1, row_count):
                second_copy(group, step).wait_send()

    def drain_ids(slot, carry):
        ids_copy(slot).wait_send()
        return carry

    def drain_rows(slot, carry):
        rows_copy(slot).wait_send()
        return carry

    def drain_last(i, carry):
        last_copy(lax.rem(i, per), lax.div(i, per)).wait_send()
        return carry

    lax.fori_loop(1, count, drain_ids, 0)
    lax.fori_loop(1, last, drain_rows, 0)
    lax.fori_loop(0, per * SLICES, drain_last, 0)


def local(vectors, list_ids, pq_codes, fill_counts, centroids, codebook):
    row_count = lax.axis_size("row")
    col_count = lax.axis_size("col")
    count = row_count * col_count
    slot_count, feature_width = vectors.shape
    sub_total = pq_codes.shape[1]
    sub_width, code_count = codebook.shape[1:]
    per = LANES * count // slot_count
    vmem = pl.BlockSpec(memory_space=pltpu.VMEM)
    smem = pl.BlockSpec(memory_space=pltpu.SMEM)
    hbm = pl.BlockSpec(memory_space=pl.ANY)
    coded, best, live = pl.pallas_call(
        functools.partial(exchange_kernel, row_count, col_count),
        out_shape=[jax.ShapeDtypeStruct((1, slot_count), kind) for kind in (F32, F32, jnp.int32)],
        in_specs=[hbm] * 4 + [vmem, smem],
        out_specs=[vmem] * 3,
        scratch_shapes=[
            pltpu.VMEM((slot_count, feature_width), F32),
            pltpu.VMEM((slot_count, feature_width), F32),
            pltpu.VMEM((slot_count, feature_width), F32),
            pltpu.VMEM(centroids.shape, F32),
            pltpu.VMEM((sub_total, slot_count), jnp.int32),
            pltpu.VMEM((sub_total, sub_width, code_count), F32),
            pltpu.VMEM((sub_total // 2, code_count, 2 * DEPTH), BF16),
            pltpu.VMEM((feature_width, LANES), F32),
            pltpu.SMEM((count, LANES), jnp.int32),
            pltpu.SemaphoreType.DMA((5,)),
            pltpu.SemaphoreType.DMA((count,)),
            pltpu.SemaphoreType.DMA((count,)),
            pltpu.SemaphoreType.DMA((col_count // 2,)),
            pltpu.SemaphoreType.DMA((col_count // 2,)),
            pltpu.SemaphoreType.DMA((col_count // row_count, row_count)),
            pltpu.SemaphoreType.DMA((col_count,)),
            pltpu.SemaphoreType.DMA((count,)),
            pltpu.SemaphoreType.DMA((count,)),
            pltpu.SemaphoreType.DMA((SLICES, per)),
            pltpu.SemaphoreType.DMA((SLICES, per)),
        ],
        compiler_params=pltpu.CompilerParams(
            collective_id=0, has_side_effects=True, vmem_limit_bytes=56 * 2**20),
        name="exchange_score",
    )(codebook, vectors, pq_codes.T, centroids, list_ids.reshape(slot_count // LANES, LANES), fill_counts)
    alive = live.reshape(slot_count) > 0
    return jnp.where(alive, coded.reshape(slot_count), 0.0), jnp.where(alive, best.reshape(slot_count), 0.0)


def solution(mesh):
    in_specs = (
        P(("row", "col"), None),
        P(("row", "col")),
        P(("row", "col"), None),
        P(("row", "col"), None),
        P(("row", "col"), None),
        P("col", None, None),
    )
    out_specs = (P(("row", "col")), P(("row", "col")))
    return jax.shard_map(local, mesh=mesh, in_specs=in_specs, out_specs=out_specs, check_vma=False)
```

```python
import functools

import jax
import jax.numpy as jnp
from jax import lax
from jax.experimental import pallas as pl
from jax.experimental.pallas import tpu as pltpu
from jax.sharding import PartitionSpec as P

F32 = jnp.float32
BF16 = jnp.bfloat16
DEPTH = 64
LANES = 128
PAIRS = 8


def xor(i, s, count):
    out = 0
    bit = 1
    while bit < count:
        out = out + bit * lax.rem(lax.div(i, bit) + lax.div(s, bit), 2)
        bit *= 2
    return out


def split3(x):
    hi = x.astype(BF16).astype(F32)
    rest = x - hi
    mid = rest.astype(BF16).astype(F32)
    return hi, mid, rest - mid


def code_rows(c):
    hi, mid, lo = split3(-2.0 * c)
    norm = jnp.sum(c * c, axis=0, keepdims=True)
    nh, nm, nl = split3(norm)
    line = lax.broadcasted_iota(jnp.int32, c.shape, 0)
    norms = jnp.where(line == 0, nh, jnp.where(line == 1, nm, jnp.where(line == 2, nl, 0.0)))
    return [hi, hi, hi, mid, mid, lo, norms, jnp.zeros_like(c)]


def build_table(cb_ref, w_ref):
    def step(i, carry):
        pieces = code_rows(cb_ref[2 * i]) + code_rows(cb_ref[2 * i + 1])
        w_ref[i] = jnp.concatenate(pieces, axis=0).T.astype(BF16)
        return carry

    lax.fori_loop(0, w_ref.shape[0], step, 0, unroll=2)


def pick(row, idx):
    low = jnp.bitwise_and(idx, LANES - 1)
    got = None
    for part in range(row.shape[1] // LANES):
        piece = jnp.take_along_axis(
            row[:, part * LANES:(part + 1) * LANES], low, axis=1, mode="promise_in_bounds"
        )
        got = piece if got is None else jnp.where(idx >= part * LANES, piece, got)
    return got


def score_step(g, carry, rt_ref, codes_ref, base, cb_ref, w_ref):
    sub_width = cb_ref.shape[1]
    ones = jnp.ones((sub_width, LANES), F32)
    zeros = jnp.zeros((sub_width, LANES), F32)
    blank = jnp.zeros((DEPTH, LANES), BF16)

    def side(m, code):
        r = rt_ref[pl.ds(pl.multiple_of(m * sub_width, sub_width), sub_width), :]
        hi, mid, lo = split3(r)
        x = jnp.concatenate([hi, mid, lo, hi, mid, hi, ones, zeros], axis=0).astype(BF16)
        diff = r - pick(cb_ref[m], jnp.broadcast_to(code, (sub_width, LANES)))
        return x, r * r, diff * diff

    coded, norm, best = carry
    codes = codes_ref[pl.ds(pl.multiple_of(g * 2 * PAIRS, 8), 2 * PAIRS), pl.ds(base, LANES)]
    for i in range(PAIRS):
        pair = g * PAIRS + i
        xa, na, da = side(2 * pair, codes[2 * i:2 * i + 1, :])
        xb, nb, db = side(2 * pair + 1, codes[2 * i + 1:2 * i + 2, :])
        x = jnp.concatenate(
            [jnp.concatenate([xa, blank], axis=1), jnp.concatenate([blank, xb], axis=1)], axis=0)
        table = jnp.dot(w_ref[pair], x, preferred_element_type=F32)
        best = best + jnp.min(table, axis=0, keepdims=True)
        norm = norm + (na + nb)
        coded = coded + (da + db)
    return coded, norm, best


def score_start(sub_width):
    zeros = jnp.zeros((sub_width, LANES), F32)
    return zeros, zeros, jnp.zeros((1, 2 * LANES), F32)


def score_end(carry):
    coded, norm, best = carry
    coded = jnp.sum(coded, axis=0, keepdims=True)
    return coded, best[:, :LANES] + best[:, LANES:] + jnp.sum(norm, axis=0, keepdims=True)


def exchange_kernel(row_count, col_count, cb_hbm, v_hbm, codes_hbm, cent_hbm, ids_ref, fill_ref,
                    coded_ref, best_ref, live_ref,
                    wanted_ref, got_ref, v_ref, cent_ref, codes_ref, book_ref, w_ref, rt_ref, ids_own, ids_sm,
                    local_sem, ready, ids_send, ids_recv, first_send, mirror_send, second_send, book_recv,
                    rows_send, rows_recv, last_send, last_recv):
    row = lax.axis_index("row")
    col = lax.axis_index("col")
    me = row * col_count + col
    count = row_count * col_count
    sub_local = cb_hbm.shape[0]
    slot_count = v_ref.shape[0]
    capacity = slot_count // count
    lists = cent_ref.shape[0]
    per = LANES // capacity
    spans = col_count // per
    steps = v_ref.shape[1] // LANES
    last = count - per
    cuts = (0, steps - steps // 3, steps)

    top = col_count // 2
    quarter = col_count // 4
    zone = lax.div(col, quarter)
    inner = zone * (3 - zone) > 0
    outer = zone * (3 - zone) == 0
    mirror = xor(col, top + quarter, col_count)
    kin = row_count * top

    def same_slot(i):
        t = lax.rem(i, top)
        return lax.div(i, top) * col_count + t + lax.div(t, quarter) * top

    def cross_slot(i):
        return lax.div(i, top) * col_count + quarter + lax.rem(i, top)

    def place(slot):
        return xor(row, lax.div(slot, col_count), row_count), xor(col, lax.rem(slot, col_count), col_count)

    def piece(j):
        return book_ref.at[pl.ds(j * sub_local, sub_local)]

    def block(ref, owner):
        return ref.at[pl.ds(pl.multiple_of(owner * capacity, capacity), capacity)]

    cent_copy = pltpu.make_async_copy(cent_hbm, cent_ref, local_sem.at[0])
    book_copy = pltpu.make_async_copy(cb_hbm, piece(col), local_sem.at[1])
    v_copy = pltpu.make_async_copy(v_hbm, v_ref, local_sem.at[2])
    codes_copy = pltpu.make_async_copy(codes_hbm, codes_ref, local_sem.at[3])
    book_copy.start()
    cent_copy.start()
    v_copy.start()
    codes_copy.start()

    barrier = pltpu.get_barrier_semaphore()

    for p in range(per):
        ids = ids_ref[...]
        ids_own[p] = ids if p == 0 else pltpu.roll(ids, LANES - p * capacity, 1)

    def signal(sem, slot):
        r, c = place(slot)
        pl.semaphore_signal(sem, inc=1, device_id=(r, c), device_id_type=pl.DeviceIdType.MESH)

    def greet_same(i, carry):
        signal(barrier, same_slot(i))
        return carry

    def greet_cross(i, carry):
        signal(barrier, cross_slot(i))
        return carry

    def tell_cross(i, carry):
        signal(ready, cross_slot(i))
        return carry

    lax.fori_loop(1, kin, greet_same, 0)

    @pl.when(inner)
    def _():
        lax.fori_loop(0, kin, greet_cross, 0)
        pl.semaphore_wait(barrier, kin - 1)

    @pl.when(outer)
    def _():
        pl.semaphore_wait(barrier, count - 1)
        lax.fori_loop(0, kin, tell_cross, 0)

    def ids_of(owner):
        return ids_own.at[lax.rem(owner, per), pl.ds(lax.div(owner, per), 1)]

    def ids_copy(slot):
        r, c = place(slot)
        return pltpu.make_async_remote_copy(
            src_ref=ids_of(r * col_count + c), dst_ref=ids_sm.at[pl.ds(me, 1)],
            send_sem=ids_send.at[slot], recv_sem=ids_recv.at[slot],
            device_id=(r, c), device_id_type=pl.DeviceIdType.MESH)

    def ids_arrived(slot):
        r, c = place(slot)
        return pltpu.make_async_remote_copy(
            src_ref=ids_of(me), dst_ref=ids_sm.at[pl.ds(r * col_count + c, 1)],
            send_sem=ids_send.at[slot], recv_sem=ids_recv.at[slot],
            device_id=(r, c), device_id_type=pl.DeviceIdType.MESH)

    def ids_same(i, carry):
        ids_copy(same_slot(kin - 1 - i)).start()
        return carry

    def ids_cross(i, carry):
        ids_copy(cross_slot(i)).start()
        return carry

    lax.fori_loop(0, kin - 1, ids_same, 0)

    @pl.when(outer)
    def _():
        lax.fori_loop(0, kin, ids_cross, 0)

    own_ids = pltpu.make_async_copy(
        ids_of(me), ids_sm.at[pl.ds(me, 1)], local_sem.at[4])
    own_ids.start()

    side = lax.rem(row, 2)
    peer = row + 1 - 2 * side

    def book_copy_to(source, target, sem):
        return pltpu.make_async_remote_copy(
            src_ref=piece(source), dst_ref=piece(source), send_sem=sem, recv_sem=book_recv.at[source],
            device_id=(row, target), device_id_type=pl.DeviceIdType.MESH)

    def peer_copy(k):
        j = 2 * k + side
        return pltpu.make_async_remote_copy(
            src_ref=piece(j), dst_ref=piece(j), send_sem=second_send.at[k], recv_sem=book_recv.at[j],
            device_id=(peer, col), device_id_type=pl.DeviceIdType.MESH)

    def arrived(j):
        return book_copy_to(j, mirror, first_send.at[0])

    def spread(source, sems, begin, end):
        return [book_copy_to(source, xor(col, b, col_count), sems.at[b]) for b in range(begin, end)]

    spreads = lax.rem(col, 2) == side
    book_copy.wait()

    @pl.when(spreads)
    def _():
        for copy in [book_copy_to(col, mirror, first_send.at[0])] + spread(col, first_send, 1, quarter):
            copy.start()

        @pl.when(outer)
        def _():
            for copy in spread(col, first_send, quarter, top):
                copy.start()

    def gather(owner, out_ref):
        out = block(out_ref, owner)
        for j in range(capacity):
            at = jnp.bitwise_and(ids_sm[owner, j], lists - 1)
            out[pl.ds(j, 1), :] = cent_ref[pl.ds(at, 1), :]

    def rows_copy(slot):
        r, c = place(slot)
        return pltpu.make_async_remote_copy(
            src_ref=block(wanted_ref, r * col_count + c), dst_ref=block(got_ref, me),
            send_sem=rows_send.at[slot], recv_sem=rows_recv.at[slot],
            device_id=(r, c), device_id_type=pl.DeviceIdType.MESH)

    def rows_arrived(slot):
        r, c = place(slot)
        return pltpu.make_async_remote_copy(
            src_ref=block(wanted_ref, me), dst_ref=block(got_ref, r * col_count + c),
            send_sem=rows_send.at[slot], recv_sem=rows_recv.at[slot],
            device_id=(r, c), device_id_type=pl.DeviceIdType.MESH)

    def last_part(f):
        return pl.ds(cuts[f] * LANES, (cuts[f + 1] - cuts[f]) * LANES)

    def last_copy(j, f):
        r, c = place(last + j)
        return pltpu.make_async_remote_copy(
            src_ref=block(wanted_ref, r * col_count + c).at[:, last_part(f)],
            dst_ref=block(got_ref, me).at[:, last_part(f)],
            send_sem=last_send.at[f, j], recv_sem=last_recv.at[f, j],
            device_id=(r, c), device_id_type=pl.DeviceIdType.MESH)

    def last_arrived(j, f):
        r, c = place(last + j)
        return pltpu.make_async_remote_copy(
            src_ref=block(wanted_ref, me).at[:, last_part(f)],
            dst_ref=block(got_ref, r * col_count + c).at[:, last_part(f)],
            send_sem=last_send.at[f, j], recv_sem=last_recv.at[f, j],
            device_id=(r, c), device_id_type=pl.DeviceIdType.MESH)

    def serve(first, end, before=None):
        def one(slot, carry):
            r, c = place(slot)
            ids_arrived(slot).wait_recv()
            gather(r * col_count + c, wanted_ref)

            @pl.when(slot > first)
            def _():
                @pl.when(slot <= last)
                def _():
                    rows_copy(slot - 1).start()

            if before is not None:
                @pl.when(slot == first)
                def _():
                    rows_copy(before).start()

            return carry

        lax.fori_loop(first, end, one, 0)
        return end - 1

    def forward():
        arrived(mirror).wait_recv()
        for copy in spread(mirror, mirror_send, 1, top):
            copy.start()

    @pl.when(outer)
    def _():
        @pl.when(spreads)
        def _():
            forward()

    cent_copy.wait()
    pending = serve(top + quarter, col_count)
    own_ids.wait()
    gather(me, got_ref)
    rows_copy(pending).start()

    @pl.when(inner)
    def _():
        pl.semaphore_wait(ready, kin)
        lax.fori_loop(0, kin, ids_cross, 0)

        @pl.when(spreads)
        def _():
            for copy in spread(col, first_send, quarter, top):
                copy.start()
            forward()

    pending = serve(1, quarter)
    for a in range(1, row_count // 2):
        pending = serve(a * col_count + top + quarter, (a + 1) * col_count, pending)
        pending = serve(a * col_count, a * col_count + quarter, pending)
    v_copy.wait()
    codes_copy.wait()
    rows_copy(pending).start()

    def pass_on(k, carry):
        j = 2 * k + side

        @pl.when((j - col) * (j - mirror) != 0)
        def _():
            arrived(j).wait_recv()

        @pl.when(j != col)
        def _():
            peer_copy(k).start()

        return carry

    lax.fori_loop(0, top, pass_on, 0)

    pending = None
    for a in range(row_count // 2):
        pending = serve(a * col_count + quarter, a * col_count + top + quarter, pending)
    serve((row_count // 2) * col_count, count, pending)

    def send_last(f):
        def one(j, carry):
            last_copy(j, f).start()
            return carry

        lax.fori_loop(0, per, one, 0)

    send_last(0)
    send_last(1)

    def from_peer(k, carry):
        j = 2 * k + 1 - side

        @pl.when(j != col)
        def _():
            arrived(j).wait_recv()

        return carry

    lax.fori_loop(0, top, from_peer, 0)
    build_table(book_ref, w_ref)

    lane = lax.broadcasted_iota(jnp.int32, (1, LANES), 1)
    sub_width = book_ref.shape[1]

    def group_at(g):
        a = lax.div(g, 2 * spans) * 2 + lax.rem(g, 2)
        h = lax.rem(lax.div(g, 2), spans)
        first = xor(row, a, row_count) * col_count + xor(lax.div(col, per), h, spans) * per
        return a * col_count + h * per, first, pl.multiple_of(first * capacity, LANES)

    def finish(carry, first, base):
        coded, best = score_end(carry)
        bound = jnp.zeros((1, LANES), jnp.int32)
        for j in range(per):
            bound = jnp.where(lane >= j * capacity, fill_ref[0, first + j] + j * capacity, bound)
        coded_ref[:, pl.ds(base, LANES)] = coded
        best_ref[:, pl.ds(base, LANES)] = best
        live_ref[:, pl.ds(base, LANES)] = jnp.where(lane < bound, 1, 0)

    def group_step(g, carry):
        slot, first, base = group_at(g)

        def settle(j, inner):
            @pl.when(slot + j > 0)
            def _():
                rows_arrived(slot + j).wait_recv()

            return inner

        lax.fori_loop(0, per, settle, 0)
        rt_ref[...] = (v_ref[pl.ds(base, LANES), :] - got_ref[pl.ds(base, LANES), :]).T

        def step(f, inner):
            return score_step(f, inner, rt_ref, codes_ref, base, book_ref, w_ref)

        finish(lax.fori_loop(0, steps, step, score_start(sub_width)), first, base)
        return carry

    lax.fori_loop(0, row_count * spans - 1, group_step, 0)

    _, first, base = group_at(row_count * spans - 1)

    carry = score_start(sub_width)
    for f in range(2):
        for j in range(per):
            last_arrived(j, f).wait_recv()
        part = last_part(f)
        rt_ref[part, :] = (v_ref[pl.ds(base, LANES), part] - got_ref[pl.ds(base, LANES), part]).T

        def last_step(g, inside):
            return score_step(g, inside, rt_ref, codes_ref, base, book_ref, w_ref)

        carry = lax.fori_loop(cuts[f], cuts[f + 1], last_step, carry)
    finish(carry, first, base)

    @pl.when(spreads)
    def _():
        book_copy_to(col, mirror, first_send.at[0]).wait_send()
        for copy in spread(col, first_send, 1, top) + spread(mirror, mirror_send, 1, top):
            copy.wait_send()

    def drain_peer(k, carry):
        @pl.when(2 * k + side != col)
        def _():
            peer_copy(k).wait_send()

        return carry

    lax.fori_loop(0, top, drain_peer, 0)

    def drain_ids(slot, carry):
        ids_copy(slot).wait_send()
        return carry

    def drain_rows(slot, carry):
        rows_copy(slot).wait_send()
        return carry

    def drain_last(j, carry):
        last_copy(j, 0).wait_send()
        last_copy(j, 1).wait_send()
        return carry

    lax.fori_loop(1, count, drain_ids, 0)
    lax.fori_loop(1, last, drain_rows, 0)
    lax.fori_loop(0, per, drain_last, 0)


def local(vectors, list_ids, pq_codes, fill_counts, centroids, codebook):
    row_count = lax.axis_size("row")
    col_count = lax.axis_size("col")
    count = row_count * col_count
    slot_count, feature_width = vectors.shape
    sub_total = pq_codes.shape[1]
    sub_width, code_count = codebook.shape[1:]
    per = LANES * count // slot_count
    vmem = pl.BlockSpec(memory_space=pltpu.VMEM)
    smem = pl.BlockSpec(memory_space=pltpu.SMEM)
    hbm = pl.BlockSpec(memory_space=pl.ANY)
    coded, best, live = pl.pallas_call(
        functools.partial(exchange_kernel, row_count, col_count),
        out_shape=[jax.ShapeDtypeStruct((1, slot_count), kind) for kind in (F32, F32, jnp.int32)],
        in_specs=[hbm] * 4 + [vmem, smem],
        out_specs=[vmem] * 3,
        scratch_shapes=[
            pltpu.VMEM((slot_count, feature_width), F32),
            pltpu.VMEM((slot_count, feature_width), F32),
            pltpu.VMEM((slot_count, feature_width), F32),
            pltpu.VMEM(centroids.shape, F32),
            pltpu.VMEM((sub_total, slot_count), jnp.int32),
            pltpu.VMEM((sub_total, sub_width, code_count), F32),
            pltpu.VMEM((sub_total // 2, code_count, 2 * DEPTH), BF16),
            pltpu.VMEM((feature_width, LANES), F32),
            pltpu.VMEM((per, slot_count // LANES, LANES), jnp.int32),
            pltpu.SMEM((count, LANES), jnp.int32),
            pltpu.SemaphoreType.DMA((5,)),
            pltpu.SemaphoreType.REGULAR,
            pltpu.SemaphoreType.DMA((count,)),
            pltpu.SemaphoreType.DMA((count,)),
            pltpu.SemaphoreType.DMA((col_count // 2,)),
            pltpu.SemaphoreType.DMA((col_count // 2,)),
            pltpu.SemaphoreType.DMA((col_count // 2,)),
            pltpu.SemaphoreType.DMA((col_count,)),
            pltpu.SemaphoreType.DMA((count,)),
            pltpu.SemaphoreType.DMA((count,)),
            pltpu.SemaphoreType.DMA((2, per)),
            pltpu.SemaphoreType.DMA((2, per)),
        ],
        compiler_params=pltpu.CompilerParams(
            collective_id=0, has_side_effects=True, vmem_limit_bytes=56 * 2**20),
        name="exchange_score",
    )(codebook, vectors, pq_codes.T, centroids, list_ids.reshape(slot_count // LANES, LANES), fill_counts)
    alive = live.reshape(slot_count) > 0
    return jnp.where(alive, coded.reshape(slot_count), 0.0), jnp.where(alive, best.reshape(slot_count), 0.0)


def solution(mesh):
    in_specs = (
        P(("row", "col"), None),
        P(("row", "col")),
        P(("row", "col"), None),
        P(("row", "col"), None),
        P(("row", "col"), None),
        P("col", None, None),
    )
    out_specs = (P(("row", "col")), P(("row", "col")))
    return jax.shard_map(local, mesh=mesh, in_specs=in_specs, out_specs=out_specs, check_vma=False)
```

```python
import functools

import jax
import jax.numpy as jnp
from jax import lax
from jax.experimental import pallas as pl
from jax.experimental.pallas import tpu as pltpu
from jax.sharding import PartitionSpec as P

F32 = jnp.float32
BF16 = jnp.bfloat16
DEPTH = 64
LANES = 128
PAIRS = 8


def xor(i, s, count):
    out = 0
    bit = 1
    while bit < count:
        out = out + bit * lax.rem(lax.div(i, bit) + lax.div(s, bit), 2)
        bit *= 2
    return out


def split3(x):
    hi = x.astype(BF16).astype(F32)
    rest = x - hi
    mid = rest.astype(BF16).astype(F32)
    return hi, mid, rest - mid


def code_rows(c):
    hi, mid, lo = split3(-2.0 * c)
    norm = jnp.sum(c * c, axis=0, keepdims=True)
    nh, nm, nl = split3(norm)
    line = lax.broadcasted_iota(jnp.int32, c.shape, 0)
    norms = jnp.where(line == 0, nh, jnp.where(line == 1, nm, jnp.where(line == 2, nl, 0.0)))
    return [hi, hi, hi, mid, mid, lo, norms, jnp.zeros_like(c)]


def build_table(cb_ref, w_ref):
    def step(i, carry):
        pieces = code_rows(cb_ref[2 * i]) + code_rows(cb_ref[2 * i + 1])
        w_ref[i] = jnp.concatenate(pieces, axis=0).T.astype(BF16)
        return carry

    lax.fori_loop(0, w_ref.shape[0], step, 0, unroll=2)


def pick(row, idx):
    low = jnp.bitwise_and(idx, LANES - 1)
    got = None
    for part in range(row.shape[1] // LANES):
        piece = jnp.take_along_axis(
            row[:, part * LANES:(part + 1) * LANES], low, axis=1, mode="promise_in_bounds"
        )
        got = piece if got is None else jnp.where(idx >= part * LANES, piece, got)
    return got


def score_step(g, carry, rt_ref, codes_ref, base, cb_ref, w_ref):
    sub_width = cb_ref.shape[1]
    ones = jnp.ones((sub_width, LANES), F32)
    zeros = jnp.zeros((sub_width, LANES), F32)
    blank = jnp.zeros((DEPTH, LANES), BF16)

    def side(m, code):
        r = rt_ref[pl.ds(pl.multiple_of(m * sub_width, sub_width), sub_width), :]
        hi, mid, lo = split3(r)
        x = jnp.concatenate([hi, mid, lo, hi, mid, hi, ones, zeros], axis=0).astype(BF16)
        diff = r - pick(cb_ref[m], jnp.broadcast_to(code, (sub_width, LANES)))
        return x, r * r, diff * diff

    coded, norm, best = carry
    codes = codes_ref[pl.ds(pl.multiple_of(g * 2 * PAIRS, 8), 2 * PAIRS), pl.ds(base, LANES)]
    for i in range(PAIRS):
        pair = g * PAIRS + i
        xa, na, da = side(2 * pair, codes[2 * i:2 * i + 1, :])
        xb, nb, db = side(2 * pair + 1, codes[2 * i + 1:2 * i + 2, :])
        x = jnp.concatenate(
            [jnp.concatenate([xa, blank], axis=1), jnp.concatenate([blank, xb], axis=1)], axis=0)
        table = jnp.dot(w_ref[pair], x, preferred_element_type=F32)
        best = best + jnp.min(table, axis=0, keepdims=True)
        norm = norm + (na + nb)
        coded = coded + (da + db)
    return coded, norm, best


def score_start(sub_width):
    zeros = jnp.zeros((sub_width, LANES), F32)
    return zeros, zeros, jnp.zeros((1, 2 * LANES), F32)


def score_end(carry):
    coded, norm, best = carry
    coded = jnp.sum(coded, axis=0, keepdims=True)
    return coded, best[:, :LANES] + best[:, LANES:] + jnp.sum(norm, axis=0, keepdims=True)


def exchange_kernel(row_count, col_count, cb_hbm, v_hbm, codes_hbm, cent_hbm, ids_hbm, fill_hbm, out_hbm,
                    wanted_ref, got_ref, v_ref, cent_ref, codes_ref, book_ref, w_ref, rt_ref, out_ref, ids_ref, ids_own, fill_ref, ids_sm,
                    local_sem, ready, ids_send, ids_recv, first_send, mirror_send, second_send, book_recv,
                    rows_send, rows_recv, last_send, last_recv):
    row = lax.axis_index("row")
    col = lax.axis_index("col")
    me = row * col_count + col
    count = row_count * col_count
    sub_local = cb_hbm.shape[0]
    slot_count = v_ref.shape[0]
    capacity = slot_count // count
    lists = cent_ref.shape[0]
    per = LANES // capacity
    spans = col_count // per
    steps = v_ref.shape[1] // LANES
    last = count - per
    cuts = (0, steps - steps // 3, steps)

    top = col_count // 2
    quarter = col_count // 4
    zone = lax.div(col, quarter)
    inner = zone * (3 - zone) > 0
    outer = zone * (3 - zone) == 0
    mirror = xor(col, top + quarter, col_count)
    kin = row_count * top

    def same_slot(i):
        t = lax.rem(i, top)
        return lax.div(i, top) * col_count + t + lax.div(t, quarter) * top

    def cross_slot(i):
        return lax.div(i, top) * col_count + quarter + lax.rem(i, top)

    def place(slot):
        return xor(row, lax.div(slot, col_count), row_count), xor(col, lax.rem(slot, col_count), col_count)

    def piece(j):
        return book_ref.at[pl.ds(j * sub_local, sub_local)]

    def block(ref, owner):
        return ref.at[pl.ds(pl.multiple_of(owner * capacity, capacity), capacity)]

    cent_copy = pltpu.make_async_copy(cent_hbm, cent_ref, local_sem.at[0])
    book_copy = pltpu.make_async_copy(cb_hbm, piece(col), local_sem.at[1])
    v_copy = pltpu.make_async_copy(v_hbm, v_ref, local_sem.at[2])
    codes_copy = pltpu.make_async_copy(codes_hbm, codes_ref, local_sem.at[3])
    ids_local = pltpu.make_async_copy(ids_hbm, ids_ref, local_sem.at[5])
    fill_copy = pltpu.make_async_copy(fill_hbm, fill_ref, local_sem.at[6])
    out_copy = pltpu.make_async_copy(out_ref, out_hbm, local_sem.at[7])
    ids_local.start()
    book_copy.start()
    cent_copy.start()
    v_copy.start()
    codes_copy.start()
    fill_copy.start()

    barrier = pltpu.get_barrier_semaphore()


    def signal(sem, slot):
        r, c = place(slot)
        pl.semaphore_signal(sem, inc=1, device_id=(r, c), device_id_type=pl.DeviceIdType.MESH)

    def greet_same(i, carry):
        signal(barrier, same_slot(i))
        return carry

    def greet_cross(i, carry):
        signal(barrier, cross_slot(i))
        return carry

    def tell_cross(i, carry):
        signal(ready, cross_slot(i))
        return carry

    def shift_ids():
        ids_local.wait()
        for p in range(per):
            ids = ids_ref[...]
            ids_own[p] = ids if p == 0 else pltpu.roll(ids, LANES - p * capacity, 1)

    lax.fori_loop(1, kin, greet_same, 0)

    @pl.when(inner)
    def _():
        lax.fori_loop(0, kin, greet_cross, 0)

    shift_ids()

    @pl.when(inner)
    def _():
        pl.semaphore_wait(barrier, kin - 1)

    @pl.when(outer)
    def _():
        pl.semaphore_wait(barrier, count - 1)
        lax.fori_loop(0, kin, tell_cross, 0)

    def ids_of(owner):
        return ids_own.at[lax.rem(owner, per), pl.ds(lax.div(owner, per), 1)]

    def ids_copy(slot):
        r, c = place(slot)
        return pltpu.make_async_remote_copy(
            src_ref=ids_of(r * col_count + c), dst_ref=ids_sm.at[pl.ds(me, 1)],
            send_sem=ids_send.at[slot], recv_sem=ids_recv.at[slot],
            device_id=(r, c), device_id_type=pl.DeviceIdType.MESH)

    def ids_arrived(slot):
        r, c = place(slot)
        return pltpu.make_async_remote_copy(
            src_ref=ids_of(me), dst_ref=ids_sm.at[pl.ds(r * col_count + c, 1)],
            send_sem=ids_send.at[slot], recv_sem=ids_recv.at[slot],
            device_id=(r, c), device_id_type=pl.DeviceIdType.MESH)

    def ids_same(i, carry):
        ids_copy(same_slot(kin - 1 - i)).start()
        return carry

    def ids_cross(i, carry):
        ids_copy(cross_slot(i)).start()
        return carry

    lax.fori_loop(0, kin - 1, ids_same, 0)

    @pl.when(outer)
    def _():
        lax.fori_loop(0, kin, ids_cross, 0)

    own_ids = pltpu.make_async_copy(
        ids_of(me), ids_sm.at[pl.ds(me, 1)], local_sem.at[4])
    own_ids.start()

    side = lax.rem(row, 2)
    peer = row + 1 - 2 * side

    def book_copy_to(source, target, sem):
        return pltpu.make_async_remote_copy(
            src_ref=piece(source), dst_ref=piece(source), send_sem=sem, recv_sem=book_recv.at[source],
            device_id=(row, target), device_id_type=pl.DeviceIdType.MESH)

    def peer_copy(k):
        j = 2 * k + side
        return pltpu.make_async_remote_copy(
            src_ref=piece(j), dst_ref=piece(j), send_sem=second_send.at[k], recv_sem=book_recv.at[j],
            device_id=(peer, col), device_id_type=pl.DeviceIdType.MESH)

    def arrived(j):
        return book_copy_to(j, mirror, first_send.at[0])

    def spread(source, sems, begin, end):
        return [book_copy_to(source, xor(col, b, col_count), sems.at[b]) for b in range(begin, end)]

    spreads = lax.rem(col, 2) == side
    book_copy.wait()

    @pl.when(spreads)
    def _():
        for copy in [book_copy_to(col, mirror, first_send.at[0])] + spread(col, first_send, 1, quarter):
            copy.start()

        @pl.when(outer)
        def _():
            for copy in spread(col, first_send, quarter, top):
                copy.start()

    def gather(owner, out_ref):
        out = block(out_ref, owner)
        for j in range(capacity):
            at = jnp.bitwise_and(ids_sm[owner, j], lists - 1)
            out[pl.ds(j, 1), :] = cent_ref[pl.ds(at, 1), :]

    def rows_copy(slot):
        r, c = place(slot)
        return pltpu.make_async_remote_copy(
            src_ref=block(wanted_ref, r * col_count + c), dst_ref=block(got_ref, me),
            send_sem=rows_send.at[slot], recv_sem=rows_recv.at[slot],
            device_id=(r, c), device_id_type=pl.DeviceIdType.MESH)

    def rows_arrived(slot):
        r, c = place(slot)
        return pltpu.make_async_remote_copy(
            src_ref=block(wanted_ref, me), dst_ref=block(got_ref, r * col_count + c),
            send_sem=rows_send.at[slot], recv_sem=rows_recv.at[slot],
            device_id=(r, c), device_id_type=pl.DeviceIdType.MESH)

    def last_part(f):
        return pl.ds(cuts[f] * LANES, (cuts[f + 1] - cuts[f]) * LANES)

    def last_copy(j, f):
        r, c = place(last + j)
        return pltpu.make_async_remote_copy(
            src_ref=block(wanted_ref, r * col_count + c).at[:, last_part(f)],
            dst_ref=block(got_ref, me).at[:, last_part(f)],
            send_sem=last_send.at[f, j], recv_sem=last_recv.at[f, j],
            device_id=(r, c), device_id_type=pl.DeviceIdType.MESH)

    def last_arrived(j, f):
        r, c = place(last + j)
        return pltpu.make_async_remote_copy(
            src_ref=block(wanted_ref, me).at[:, last_part(f)],
            dst_ref=block(got_ref, r * col_count + c).at[:, last_part(f)],
            send_sem=last_send.at[f, j], recv_sem=last_recv.at[f, j],
            device_id=(r, c), device_id_type=pl.DeviceIdType.MESH)

    def serve(first, end, before=None):
        def one(slot, carry):
            r, c = place(slot)
            ids_arrived(slot).wait_recv()
            gather(r * col_count + c, wanted_ref)

            @pl.when(slot > first)
            def _():
                @pl.when(slot <= last)
                def _():
                    rows_copy(slot - 1).start()

            if before is not None:
                @pl.when(slot == first)
                def _():
                    rows_copy(before).start()

            return carry

        lax.fori_loop(first, end, one, 0)
        return end - 1

    def forward():
        arrived(mirror).wait_recv()
        for copy in spread(mirror, mirror_send, 1, top):
            copy.start()

    @pl.when(outer)
    def _():
        @pl.when(spreads)
        def _():
            forward()

    cent_copy.wait()
    pending = serve(top + quarter, col_count)
    own_ids.wait()
    gather(me, got_ref)
    rows_copy(pending).start()

    @pl.when(inner)
    def _():
        pl.semaphore_wait(ready, kin)
        lax.fori_loop(0, kin, ids_cross, 0)

        @pl.when(spreads)
        def _():
            for copy in spread(col, first_send, quarter, top):
                copy.start()
            forward()

    pending = serve(1, quarter)
    for a in range(1, row_count // 2):
        pending = serve(a * col_count + top + quarter, (a + 1) * col_count, pending)
        pending = serve(a * col_count, a * col_count + quarter, pending)
    v_copy.wait()
    codes_copy.wait()
    rows_copy(pending).start()

    def pass_on(k, carry):
        j = 2 * k + side

        @pl.when((j - col) * (j - mirror) != 0)
        def _():
            arrived(j).wait_recv()

        @pl.when(j != col)
        def _():
            peer_copy(k).start()

        return carry

    lax.fori_loop(0, top, pass_on, 0)

    pending = None
    for a in range(row_count // 2):
        pending = serve(a * col_count + quarter, a * col_count + top + quarter, pending)
    serve((row_count // 2) * col_count, count, pending)

    def send_last(f):
        def one(j, carry):
            last_copy(j, f).start()
            return carry

        lax.fori_loop(0, per, one, 0)

    send_last(0)
    send_last(1)

    def from_peer(k, carry):
        j = 2 * k + 1 - side

        @pl.when(j != col)
        def _():
            arrived(j).wait_recv()

        return carry

    lax.fori_loop(0, top, from_peer, 0)
    build_table(book_ref, w_ref)

    lane = lax.broadcasted_iota(jnp.int32, (1, LANES), 1)
    sub_width = book_ref.shape[1]

    def group_at(g):
        a = lax.div(g, 2 * spans) * 2 + lax.rem(g, 2)
        h = lax.rem(lax.div(g, 2), spans)
        first = xor(row, a, row_count) * col_count + xor(lax.div(col, per), h, spans) * per
        return a * col_count + h * per, first, pl.multiple_of(first * capacity, LANES)

    def finish(carry, first, base):
        coded, best = score_end(carry)
        bound = jnp.zeros((1, LANES), jnp.int32)
        for j in range(per):
            bound = jnp.where(lane >= j * capacity, fill_ref[0, first + j] + j * capacity, bound)
        out_ref[0:1, pl.ds(base, LANES)] = coded
        out_ref[1:2, pl.ds(base, LANES)] = best
        out_ref[2:3, pl.ds(base, LANES)] = jnp.where(lane < bound, 1.0, 0.0)

    def group_step(g, carry):
        slot, first, base = group_at(g)

        def settle(j, inner):
            @pl.when(slot + j > 0)
            def _():
                rows_arrived(slot + j).wait_recv()

            return inner

        lax.fori_loop(0, per, settle, 0)
        rt_ref[...] = (v_ref[pl.ds(base, LANES), :] - got_ref[pl.ds(base, LANES), :]).T

        def step(f, inner):
            return score_step(f, inner, rt_ref, codes_ref, base, book_ref, w_ref)

        finish(lax.fori_loop(0, steps, step, score_start(sub_width)), first, base)
        return carry

    fill_copy.wait()
    lax.fori_loop(0, row_count * spans - 1, group_step, 0)

    def sent(src, sem):
        return pltpu.make_async_remote_copy(
            src_ref=src, dst_ref=src, send_sem=sem, recv_sem=ids_recv.at[0],
            device_id=(row, mirror), device_id_type=pl.DeviceIdType.MESH)

    def drain_ids(slot, carry):
        sent(ids_own.at[0, pl.ds(0, 1)], ids_send.at[slot]).wait_send()
        return carry

    def drain_rows(slot, carry):
        sent(block(wanted_ref, 0), rows_send.at[slot]).wait_send()
        return carry

    def drain_last(j, carry):
        for f in range(2):
            sent(block(wanted_ref, 0).at[:, last_part(f)], last_send.at[f, j]).wait_send()
        return carry

    lax.fori_loop(1, count, drain_ids, 0)
    lax.fori_loop(1, (row_count // 2) * col_count, drain_rows, 0)

    _, first, base = group_at(row_count * spans - 1)

    carry = score_start(sub_width)
    for f in range(2):
        for j in range(per):
            last_arrived(j, f).wait_recv()
        part = last_part(f)
        rt_ref[part, :] = (v_ref[pl.ds(base, LANES), part] - got_ref[pl.ds(base, LANES), part]).T

        def last_step(g, inside):
            return score_step(g, inside, rt_ref, codes_ref, base, book_ref, w_ref)

        carry = lax.fori_loop(cuts[f], cuts[f + 1], last_step, carry)
    finish(carry, first, base)

    @pl.when(spreads)
    def _():
        book_copy_to(col, mirror, first_send.at[0]).wait_send()
        for copy in spread(col, first_send, 1, top) + spread(mirror, mirror_send, 1, top):
            copy.wait_send()

    def drain_peer(k, carry):
        @pl.when(2 * k + side != col)
        def _():
            peer_copy(k).wait_send()

        return carry

    lax.fori_loop(0, top, drain_peer, 0)

    lax.fori_loop((row_count // 2) * col_count, last, drain_rows, 0)
    lax.fori_loop(0, per, drain_last, 0)
    out_copy.start()
    out_copy.wait()


def local(vectors, list_ids, pq_codes, fill_counts, centroids, codebook):
    row_count = lax.axis_size("row")
    col_count = lax.axis_size("col")
    count = row_count * col_count
    slot_count, feature_width = vectors.shape
    sub_total = pq_codes.shape[1]
    sub_width, code_count = codebook.shape[1:]
    per = LANES * count // slot_count
    hbm = pl.BlockSpec(memory_space=pl.ANY)
    coded, best, live = pl.pallas_call(
        functools.partial(exchange_kernel, row_count, col_count),
        out_shape=jax.ShapeDtypeStruct((3, slot_count), F32),
        in_specs=[hbm] * 6,
        out_specs=hbm,
        scratch_shapes=[
            pltpu.VMEM((slot_count, feature_width), F32),
            pltpu.VMEM((slot_count, feature_width), F32),
            pltpu.VMEM((slot_count, feature_width), F32),
            pltpu.VMEM(centroids.shape, F32),
            pltpu.VMEM((sub_total, slot_count), jnp.int32),
            pltpu.VMEM((sub_total, sub_width, code_count), F32),
            pltpu.VMEM((sub_total // 2, code_count, 2 * DEPTH), BF16),
            pltpu.VMEM((feature_width, LANES), F32),
            pltpu.VMEM((3, slot_count), F32),
            pltpu.VMEM((slot_count // LANES, LANES), jnp.int32),
            pltpu.VMEM((per, slot_count // LANES, LANES), jnp.int32),
            pltpu.SMEM(fill_counts.shape, jnp.int32),
            pltpu.SMEM((count, LANES), jnp.int32),
            pltpu.SemaphoreType.DMA((8,)),
            pltpu.SemaphoreType.REGULAR,
            pltpu.SemaphoreType.DMA((count,)),
            pltpu.SemaphoreType.DMA((count,)),
            pltpu.SemaphoreType.DMA((col_count // 2,)),
            pltpu.SemaphoreType.DMA((col_count // 2,)),
            pltpu.SemaphoreType.DMA((col_count // 2,)),
            pltpu.SemaphoreType.DMA((col_count,)),
            pltpu.SemaphoreType.DMA((count,)),
            pltpu.SemaphoreType.DMA((count,)),
            pltpu.SemaphoreType.DMA((2, per)),
            pltpu.SemaphoreType.DMA((2, per)),
        ],
        compiler_params=pltpu.CompilerParams(
            collective_id=0, has_side_effects=True, vmem_limit_bytes=56 * 2**20),
        name="exchange_score",
    )(codebook, vectors, pq_codes.T, centroids, list_ids.reshape(slot_count // LANES, LANES), fill_counts)
    return jnp.where(live > 0.0, coded, 0.0), jnp.where(live > 0.0, best, 0.0)


def solution(mesh):
    in_specs = (
        P(("row", "col"), None),
        P(("row", "col")),
        P(("row", "col"), None),
        P(("row", "col"), None),
        P(("row", "col"), None),
        P("col", None, None),
    )
    out_specs = (P(("row", "col")), P(("row", "col")))
    return jax.shard_map(local, mesh=mesh, in_specs=in_specs, out_specs=out_specs, check_vma=False)
```

```python
import functools

import jax
import jax.numpy as jnp
from jax import lax
from jax.experimental import pallas as pl
from jax.experimental.pallas import tpu as pltpu
from jax.sharding import PartitionSpec as P

F32 = jnp.float32
BF16 = jnp.bfloat16
DEPTH = 64
LANES = 128
PAIRS = 16


def xor(i, s, count):
    out = 0
    bit = 1
    while bit < count:
        out = out + bit * lax.rem(lax.div(i, bit) + lax.div(s, bit), 2)
        bit *= 2
    return out


def split3(x):
    hi = x.astype(BF16).astype(F32)
    rest = x - hi
    mid = rest.astype(BF16).astype(F32)
    return hi, mid, rest - mid


def code_rows(c):
    hi, mid, lo = split3(-2.0 * c)
    norm = jnp.sum(c * c, axis=0, keepdims=True)
    nh, nm, nl = split3(norm)
    line = lax.broadcasted_iota(jnp.int32, c.shape, 0)
    norms = jnp.where(line == 0, nh, jnp.where(line == 1, nm, jnp.where(line == 2, nl, 0.0)))
    return [hi, hi, hi, mid, mid, lo, norms, jnp.zeros_like(c)]


def build_table(cb_ref, w_ref):
    def step(i, carry):
        pieces = code_rows(cb_ref[2 * i]) + code_rows(cb_ref[2 * i + 1])
        w_ref[i] = jnp.concatenate(pieces, axis=0).T.astype(BF16)
        return carry

    lax.fori_loop(0, w_ref.shape[0], step, 0, unroll=2)


def pick(row, idx):
    low = jnp.bitwise_and(idx, LANES - 1)
    got = None
    for part in range(row.shape[1] // LANES):
        piece = jnp.take_along_axis(
            row[:, part * LANES:(part + 1) * LANES], low, axis=1, mode="promise_in_bounds"
        )
        got = piece if got is None else jnp.where(idx >= part * LANES, piece, got)
    return got


def score_step(g, carry, rt_ref, codes_ref, base, cb_ref, w_ref):
    sub_width = cb_ref.shape[1]
    ones = jnp.ones((sub_width, LANES), F32)
    zeros = jnp.zeros((sub_width, LANES), F32)
    blank = jnp.zeros((DEPTH, LANES), BF16)

    def side(m, code):
        r = rt_ref[pl.ds(pl.multiple_of(m * sub_width, sub_width), sub_width), :]
        hi, mid, lo = split3(r)
        x = jnp.concatenate([hi, mid, lo, hi, mid, hi, ones, zeros], axis=0).astype(BF16)
        diff = r - pick(cb_ref[m], jnp.broadcast_to(code, (sub_width, LANES)))
        return x, r * r, diff * diff

    coded, norm, best = carry
    codes = codes_ref[pl.ds(pl.multiple_of(g * 2 * PAIRS, 8), 2 * PAIRS), pl.ds(base, LANES)]
    for i in range(PAIRS):
        pair = g * PAIRS + i
        xa, na, da = side(2 * pair, codes[2 * i:2 * i + 1, :])
        xb, nb, db = side(2 * pair + 1, codes[2 * i + 1:2 * i + 2, :])
        x = jnp.concatenate(
            [jnp.concatenate([xa, blank], axis=1), jnp.concatenate([blank, xb], axis=1)], axis=0)
        table = jnp.dot(w_ref[pair], x, preferred_element_type=F32)
        best = best + jnp.min(table, axis=0, keepdims=True)
        norm = norm + (na + nb)
        coded = coded + (da + db)
    return coded, norm, best


def score_start(sub_width):
    zeros = jnp.zeros((sub_width, LANES), F32)
    return zeros, zeros, jnp.zeros((1, 2 * LANES), F32)


def score_end(carry):
    coded, norm, best = carry
    coded = jnp.sum(coded, axis=0, keepdims=True)
    return coded, best[:, :LANES] + best[:, LANES:] + jnp.sum(norm, axis=0, keepdims=True)


def exchange_kernel(row_count, col_count, cb_hbm, v_hbm, codes_hbm, cent_hbm, ids_hbm, fill_hbm, out_hbm,
                    wanted_ref, got_ref, v_ref, cent_ref, codes_ref, book_ref, w_ref, rt_ref, out_ref, ids_ref, ids_own, fill_ref, ids_sm,
                    local_sem, ready, ids_send, ids_recv, first_send, mirror_send, second_send, book_recv,
                    rows_send, rows_recv, last_send, last_recv):
    row = lax.axis_index("row")
    col = lax.axis_index("col")
    me = row * col_count + col
    count = row_count * col_count
    sub_local = cb_hbm.shape[0]
    slot_count = v_ref.shape[0]
    capacity = slot_count // count
    lists = cent_ref.shape[0]
    per = LANES // capacity
    spans = col_count // per
    width = 2 * PAIRS * cb_hbm.shape[1]
    steps = v_ref.shape[1] // width
    last = count - per
    cuts = (0, steps - steps // 3, steps)

    top = col_count // 2
    quarter = col_count // 4
    zone = lax.div(col, quarter)
    inner = zone * (3 - zone) > 0
    outer = zone * (3 - zone) == 0
    mirror = xor(col, top + quarter, col_count)
    kin = row_count * top

    def same_slot(i):
        t = lax.rem(i, top)
        return lax.div(i, top) * col_count + t + lax.div(t, quarter) * top

    def cross_slot(i):
        return lax.div(i, top) * col_count + quarter + lax.rem(i, top)

    def place(slot):
        return xor(row, lax.div(slot, col_count), row_count), xor(col, lax.rem(slot, col_count), col_count)

    def piece(j):
        return book_ref.at[pl.ds(j * sub_local, sub_local)]

    def block(ref, owner):
        return ref.at[pl.ds(pl.multiple_of(owner * capacity, capacity), capacity)]

    cent_copy = pltpu.make_async_copy(cent_hbm, cent_ref, local_sem.at[0])
    book_copy = pltpu.make_async_copy(cb_hbm, piece(col), local_sem.at[1])
    v_copy = pltpu.make_async_copy(v_hbm, v_ref, local_sem.at[2])
    codes_copy = pltpu.make_async_copy(codes_hbm, codes_ref, local_sem.at[3])
    ids_local = pltpu.make_async_copy(ids_hbm, ids_ref, local_sem.at[5])
    fill_copy = pltpu.make_async_copy(fill_hbm, fill_ref, local_sem.at[6])
    out_copy = pltpu.make_async_copy(out_ref, out_hbm, local_sem.at[7])
    ids_local.start()
    book_copy.start()
    cent_copy.start()
    v_copy.start()
    codes_copy.start()
    fill_copy.start()

    barrier = pltpu.get_barrier_semaphore()


    def signal(sem, slot):
        r, c = place(slot)
        pl.semaphore_signal(sem, inc=1, device_id=(r, c), device_id_type=pl.DeviceIdType.MESH)

    def greet_same(i, carry):
        signal(barrier, same_slot(i))
        return carry

    def greet_cross(i, carry):
        signal(barrier, cross_slot(i))
        return carry

    def tell_cross(i, carry):
        signal(ready, cross_slot(i))
        return carry

    def shift_ids():
        ids_local.wait()
        for p in range(per):
            ids = ids_ref[...]
            ids_own[p] = ids if p == 0 else pltpu.roll(ids, LANES - p * capacity, 1)

    lax.fori_loop(1, kin, greet_same, 0)

    @pl.when(inner)
    def _():
        lax.fori_loop(0, kin, greet_cross, 0)

    shift_ids()

    @pl.when(inner)
    def _():
        pl.semaphore_wait(barrier, kin - 1)

    @pl.when(outer)
    def _():
        pl.semaphore_wait(barrier, count - 1)
        lax.fori_loop(0, kin, tell_cross, 0)

    def ids_of(owner):
        return ids_own.at[lax.rem(owner, per), pl.ds(lax.div(owner, per), 1)]

    def ids_copy(slot):
        r, c = place(slot)
        return pltpu.make_async_remote_copy(
            src_ref=ids_of(r * col_count + c), dst_ref=ids_sm.at[pl.ds(me, 1)],
            send_sem=ids_send.at[slot], recv_sem=ids_recv.at[slot],
            device_id=(r, c), device_id_type=pl.DeviceIdType.MESH)

    def ids_arrived(slot):
        r, c = place(slot)
        return pltpu.make_async_remote_copy(
            src_ref=ids_of(me), dst_ref=ids_sm.at[pl.ds(r * col_count + c, 1)],
            send_sem=ids_send.at[slot], recv_sem=ids_recv.at[slot],
            device_id=(r, c), device_id_type=pl.DeviceIdType.MESH)

    def ids_same(i, carry):
        ids_copy(same_slot(kin - 1 - i)).start()
        return carry

    def ids_cross(i, carry):
        ids_copy(cross_slot(i)).start()
        return carry

    lax.fori_loop(0, kin - 1, ids_same, 0)

    @pl.when(outer)
    def _():
        lax.fori_loop(0, kin, ids_cross, 0)

    own_ids = pltpu.make_async_copy(
        ids_of(me), ids_sm.at[pl.ds(me, 1)], local_sem.at[4])
    own_ids.start()

    side = lax.rem(row, 2)
    peer = row + 1 - 2 * side

    def book_copy_to(source, target, sem):
        return pltpu.make_async_remote_copy(
            src_ref=piece(source), dst_ref=piece(source), send_sem=sem, recv_sem=book_recv.at[source],
            device_id=(row, target), device_id_type=pl.DeviceIdType.MESH)

    def peer_copy(k):
        j = 2 * k + side
        return pltpu.make_async_remote_copy(
            src_ref=piece(j), dst_ref=piece(j), send_sem=second_send.at[k], recv_sem=book_recv.at[j],
            device_id=(peer, col), device_id_type=pl.DeviceIdType.MESH)

    def arrived(j):
        return book_copy_to(j, mirror, first_send.at[0])

    def spread(source, sems, begin, end):
        return [book_copy_to(source, xor(col, b, col_count), sems.at[b]) for b in range(begin, end)]

    spreads = lax.rem(col, 2) == side
    book_copy.wait()

    @pl.when(spreads)
    def _():
        for copy in [book_copy_to(col, mirror, first_send.at[0])] + spread(col, first_send, 1, quarter):
            copy.start()

        @pl.when(outer)
        def _():
            for copy in spread(col, first_send, quarter, top):
                copy.start()

    def gather(owner, out_ref):
        out = block(out_ref, owner)
        for j in range(capacity):
            at = jnp.bitwise_and(ids_sm[owner, j], lists - 1)
            out[pl.ds(j, 1), :] = cent_ref[pl.ds(at, 1), :]

    def rows_copy(slot):
        r, c = place(slot)
        return pltpu.make_async_remote_copy(
            src_ref=block(wanted_ref, r * col_count + c), dst_ref=block(got_ref, me),
            send_sem=rows_send.at[slot], recv_sem=rows_recv.at[slot],
            device_id=(r, c), device_id_type=pl.DeviceIdType.MESH)

    def rows_arrived(slot):
        r, c = place(slot)
        return pltpu.make_async_remote_copy(
            src_ref=block(wanted_ref, me), dst_ref=block(got_ref, r * col_count + c),
            send_sem=rows_send.at[slot], recv_sem=rows_recv.at[slot],
            device_id=(r, c), device_id_type=pl.DeviceIdType.MESH)

    def last_part(f):
        return pl.ds(cuts[f] * width, (cuts[f + 1] - cuts[f]) * width)

    def last_copy(j, f):
        r, c = place(last + j)
        return pltpu.make_async_remote_copy(
            src_ref=block(wanted_ref, r * col_count + c).at[:, last_part(f)],
            dst_ref=block(got_ref, me).at[:, last_part(f)],
            send_sem=last_send.at[f, j], recv_sem=last_recv.at[f, j],
            device_id=(r, c), device_id_type=pl.DeviceIdType.MESH)

    def last_arrived(j, f):
        r, c = place(last + j)
        return pltpu.make_async_remote_copy(
            src_ref=block(wanted_ref, me).at[:, last_part(f)],
            dst_ref=block(got_ref, r * col_count + c).at[:, last_part(f)],
            send_sem=last_send.at[f, j], recv_sem=last_recv.at[f, j],
            device_id=(r, c), device_id_type=pl.DeviceIdType.MESH)

    def serve(first, end, before=None):
        def one(slot, carry):
            r, c = place(slot)
            ids_arrived(slot).wait_recv()
            gather(r * col_count + c, wanted_ref)

            @pl.when(slot > first)
            def _():
                @pl.when(slot <= last)
                def _():
                    rows_copy(slot - 1).start()

            if before is not None:
                @pl.when(slot == first)
                def _():
                    rows_copy(before).start()

            return carry

        lax.fori_loop(first, end, one, 0)
        return end - 1

    def forward():
        arrived(mirror).wait_recv()
        for copy in spread(mirror, mirror_send, 1, top):
            copy.start()

    @pl.when(outer)
    def _():
        @pl.when(spreads)
        def _():
            forward()

    cent_copy.wait()
    pending = serve(top + quarter, col_count)
    own_ids.wait()
    gather(me, got_ref)
    rows_copy(pending).start()

    @pl.when(inner)
    def _():
        pl.semaphore_wait(ready, kin)
        lax.fori_loop(0, kin, ids_cross, 0)

        @pl.when(spreads)
        def _():
            for copy in spread(col, first_send, quarter, top):
                copy.start()
            forward()

    pending = serve(1, quarter)
    for a in range(1, row_count // 2):
        pending = serve(a * col_count + top + quarter, (a + 1) * col_count, pending)
        pending = serve(a * col_count, a * col_count + quarter, pending)
    v_copy.wait()
    codes_copy.wait()
    rows_copy(pending).start()

    def pass_on(k, carry):
        j = 2 * k + side

        @pl.when((j - col) * (j - mirror) != 0)
        def _():
            arrived(j).wait_recv()

        @pl.when(j != col)
        def _():
            peer_copy(k).start()

        return carry

    lax.fori_loop(0, top, pass_on, 0)

    pending = None
    for a in range(row_count // 2):
        pending = serve(a * col_count + quarter, a * col_count + top + quarter, pending)
    serve((row_count // 2) * col_count, count, pending)

    def send_last(f):
        def one(j, carry):
            last_copy(j, f).start()
            return carry

        lax.fori_loop(0, per, one, 0)

    send_last(0)
    send_last(1)

    def from_peer(k, carry):
        j = 2 * k + 1 - side

        @pl.when(j != col)
        def _():
            arrived(j).wait_recv()

        return carry

    lax.fori_loop(0, top, from_peer, 0)
    build_table(book_ref, w_ref)

    lane = lax.broadcasted_iota(jnp.int32, (1, LANES), 1)
    sub_width = book_ref.shape[1]

    def group_at(g):
        a = lax.div(g, 2 * spans) * 2 + lax.rem(g, 2)
        h = lax.rem(lax.div(g, 2), spans)
        first = xor(row, a, row_count) * col_count + xor(lax.div(col, per), h, spans) * per
        return a * col_count + h * per, first, pl.multiple_of(first * capacity, LANES)

    def finish(carry, first, base):
        coded, best = score_end(carry)
        bound = jnp.zeros((1, LANES), jnp.int32)
        for j in range(per):
            bound = jnp.where(lane >= j * capacity, fill_ref[0, first + j] + j * capacity, bound)
        out_ref[0:1, pl.ds(base, LANES)] = coded
        out_ref[1:2, pl.ds(base, LANES)] = best
        out_ref[2:3, pl.ds(base, LANES)] = jnp.where(lane < bound, 1.0, 0.0)

    def group_step(g, carry):
        slot, first, base = group_at(g)

        def settle(j, inner):
            @pl.when(slot + j > 0)
            def _():
                rows_arrived(slot + j).wait_recv()

            return inner

        lax.fori_loop(0, per, settle, 0)
        rt_ref[...] = (v_ref[pl.ds(base, LANES), :] - got_ref[pl.ds(base, LANES), :]).T

        def step(f, inner):
            return score_step(f, inner, rt_ref, codes_ref, base, book_ref, w_ref)

        finish(lax.fori_loop(0, steps, step, score_start(sub_width)), first, base)
        return carry

    fill_copy.wait()
    lax.fori_loop(0, row_count * spans - 1, group_step, 0)

    def sent(src, sem):
        return pltpu.make_async_remote_copy(
            src_ref=src, dst_ref=src, send_sem=sem, recv_sem=ids_recv.at[0],
            device_id=(row, mirror), device_id_type=pl.DeviceIdType.MESH)

    def drain_ids(slot, carry):
        sent(ids_own.at[0, pl.ds(0, 1)], ids_send.at[slot]).wait_send()
        return carry

    def drain_rows(slot, carry):
        sent(block(wanted_ref, 0), rows_send.at[slot]).wait_send()
        return carry

    def drain_last(j, carry):
        for f in range(2):
            sent(block(wanted_ref, 0).at[:, last_part(f)], last_send.at[f, j]).wait_send()
        return carry

    lax.fori_loop(1, count, drain_ids, 0)
    lax.fori_loop(1, (row_count // 2) * col_count, drain_rows, 0)

    _, first, base = group_at(row_count * spans - 1)

    carry = score_start(sub_width)
    for f in range(2):
        for j in range(per):
            last_arrived(j, f).wait_recv()
        part = last_part(f)
        rt_ref[part, :] = (v_ref[pl.ds(base, LANES), part] - got_ref[pl.ds(base, LANES), part]).T

        def last_step(g, inside):
            return score_step(g, inside, rt_ref, codes_ref, base, book_ref, w_ref)

        carry = lax.fori_loop(cuts[f], cuts[f + 1], last_step, carry)
    finish(carry, first, base)

    @pl.when(spreads)
    def _():
        book_copy_to(col, mirror, first_send.at[0]).wait_send()
        for copy in spread(col, first_send, 1, top) + spread(mirror, mirror_send, 1, top):
            copy.wait_send()

    def drain_peer(k, carry):
        @pl.when(2 * k + side != col)
        def _():
            peer_copy(k).wait_send()

        return carry

    lax.fori_loop(0, top, drain_peer, 0)

    lax.fori_loop((row_count // 2) * col_count, last, drain_rows, 0)
    lax.fori_loop(0, per, drain_last, 0)
    out_copy.start()
    out_copy.wait()


def local(vectors, list_ids, pq_codes, fill_counts, centroids, codebook):
    row_count = lax.axis_size("row")
    col_count = lax.axis_size("col")
    count = row_count * col_count
    slot_count, feature_width = vectors.shape
    sub_total = pq_codes.shape[1]
    sub_width, code_count = codebook.shape[1:]
    per = LANES * count // slot_count
    hbm = pl.BlockSpec(memory_space=pl.ANY)
    coded, best, live = pl.pallas_call(
        functools.partial(exchange_kernel, row_count, col_count),
        out_shape=jax.ShapeDtypeStruct((3, slot_count), F32),
        in_specs=[hbm] * 6,
        out_specs=hbm,
        scratch_shapes=[
            pltpu.VMEM((slot_count, feature_width), F32),
            pltpu.VMEM((slot_count, feature_width), F32),
            pltpu.VMEM((slot_count, feature_width), F32),
            pltpu.VMEM(centroids.shape, F32),
            pltpu.VMEM((sub_total, slot_count), jnp.int32),
            pltpu.VMEM((sub_total, sub_width, code_count), F32),
            pltpu.VMEM((sub_total // 2, code_count, 2 * DEPTH), BF16),
            pltpu.VMEM((feature_width, LANES), F32),
            pltpu.VMEM((3, slot_count), F32),
            pltpu.VMEM((slot_count // LANES, LANES), jnp.int32),
            pltpu.VMEM((per, slot_count // LANES, LANES), jnp.int32),
            pltpu.SMEM(fill_counts.shape, jnp.int32),
            pltpu.SMEM((count, LANES), jnp.int32),
            pltpu.SemaphoreType.DMA((8,)),
            pltpu.SemaphoreType.REGULAR,
            pltpu.SemaphoreType.DMA((count,)),
            pltpu.SemaphoreType.DMA((count,)),
            pltpu.SemaphoreType.DMA((col_count // 2,)),
            pltpu.SemaphoreType.DMA((col_count // 2,)),
            pltpu.SemaphoreType.DMA((col_count // 2,)),
            pltpu.SemaphoreType.DMA((col_count,)),
            pltpu.SemaphoreType.DMA((count,)),
            pltpu.SemaphoreType.DMA((count,)),
            pltpu.SemaphoreType.DMA((2, per)),
            pltpu.SemaphoreType.DMA((2, per)),
        ],
        compiler_params=pltpu.CompilerParams(
            collective_id=0, has_side_effects=True, vmem_limit_bytes=56 * 2**20),
        name="exchange_score",
    )(codebook, vectors, pq_codes.T, centroids, list_ids.reshape(slot_count // LANES, LANES), fill_counts)
    return jnp.where(live > 0.0, coded, 0.0), jnp.where(live > 0.0, best, 0.0)


def solution(mesh):
    in_specs = (
        P(("row", "col"), None),
        P(("row", "col")),
        P(("row", "col"), None),
        P(("row", "col"), None),
        P(("row", "col"), None),
        P("col", None, None),
    )
    out_specs = (P(("row", "col")), P(("row", "col")))
    return jax.shard_map(local, mesh=mesh, in_specs=in_specs, out_specs=out_specs, check_vma=False)
```

```python
import functools

import jax
import jax.numpy as jnp
from jax import lax
from jax.experimental import pallas as pl
from jax.experimental.pallas import tpu as pltpu
from jax.sharding import PartitionSpec as P

F32 = jnp.float32
BF16 = jnp.bfloat16
DEPTH = 64
LANES = 128
PAIRS = 16


def xor(i, s, count):
    out = 0
    bit = 1
    while bit < count:
        out = out + bit * lax.rem(lax.div(i, bit) + lax.div(s, bit), 2)
        bit *= 2
    return out


def split3(x):
    hi = x.astype(BF16).astype(F32)
    rest = x - hi
    mid = rest.astype(BF16).astype(F32)
    return hi, mid, rest - mid


def code_rows(c):
    hi, mid, lo = split3(-2.0 * c)
    norm = jnp.sum(c * c, axis=0, keepdims=True)
    nh, nm, nl = split3(norm)
    line = lax.broadcasted_iota(jnp.int32, c.shape, 0)
    norms = jnp.where(line == 0, nh, jnp.where(line == 1, nm, jnp.where(line == 2, nl, 0.0)))
    return [hi, hi, hi, mid, mid, lo, norms, jnp.zeros_like(c)]


def build_table(cb_ref, w_ref):
    def step(i, carry):
        pieces = code_rows(cb_ref[2 * i]) + code_rows(cb_ref[2 * i + 1])
        w_ref[i] = jnp.concatenate(pieces, axis=0).T.astype(BF16)
        return carry

    lax.fori_loop(0, w_ref.shape[0], step, 0, unroll=2)


def pick(row, idx):
    low = jnp.bitwise_and(idx, LANES - 1)
    got = None
    for part in range(row.shape[1] // LANES):
        piece = jnp.take_along_axis(
            row[:, part * LANES:(part + 1) * LANES], low, axis=1, mode="promise_in_bounds"
        )
        got = piece if got is None else jnp.where(idx >= part * LANES, piece, got)
    return got


def score_step(g, carry, rt_ref, codes_ref, base, cb_ref, w_ref):
    sub_width = cb_ref.shape[1]
    ones = jnp.ones((sub_width, LANES), F32)
    zeros = jnp.zeros((sub_width, LANES), F32)
    blank = jnp.zeros((DEPTH, LANES), BF16)

    def side(m, code):
        r = rt_ref[pl.ds(pl.multiple_of(m * sub_width, sub_width), sub_width), :]
        hi, mid, lo = split3(r)
        x = jnp.concatenate([hi, mid, lo, hi, mid, hi, ones, zeros], axis=0).astype(BF16)
        diff = r - pick(cb_ref[m], jnp.broadcast_to(code, (sub_width, LANES)))
        return x, r * r, diff * diff

    coded, norm, best = carry
    codes = codes_ref[pl.ds(pl.multiple_of(g * 2 * PAIRS, 8), 2 * PAIRS), pl.ds(base, LANES)]
    for i in range(PAIRS):
        pair = g * PAIRS + i
        xa, na, da = side(2 * pair, codes[2 * i:2 * i + 1, :])
        xb, nb, db = side(2 * pair + 1, codes[2 * i + 1:2 * i + 2, :])
        x = jnp.concatenate(
            [jnp.concatenate([xa, blank], axis=1), jnp.concatenate([blank, xb], axis=1)], axis=0)
        table = jnp.dot(w_ref[pair], x, preferred_element_type=F32)
        best = best + jnp.min(table, axis=0, keepdims=True)
        norm = norm + (na + nb)
        coded = coded + (da + db)
    return coded, norm, best


def score_start(sub_width):
    zeros = jnp.zeros((sub_width, LANES), F32)
    return zeros, zeros, jnp.zeros((1, 2 * LANES), F32)


def score_end(carry):
    coded, norm, best = carry
    coded = jnp.sum(coded, axis=0, keepdims=True)
    return coded, best[:, :LANES] + best[:, LANES:] + jnp.sum(norm, axis=0, keepdims=True)


def exchange_kernel(row_count, col_count, cb_hbm, v_hbm, codes_hbm, cent_hbm, ids_hbm, fill_hbm, out_hbm,
                    wanted_ref, got_ref, v_ref, cent_ref, codes_ref, book_ref, w_ref, rt_ref, out_ref, ids_ref, ids_own, fill_ref, ids_sm,
                    local_sem, ready, ids_send, ids_recv, first_send, mirror_send, second_send, book_recv,
                    rows_send, rows_recv, last_send, last_recv, out_sem):
    row = lax.axis_index("row")
    col = lax.axis_index("col")
    me = row * col_count + col
    count = row_count * col_count
    sub_local = cb_hbm.shape[0]
    slot_count = v_ref.shape[0]
    capacity = slot_count // count
    lists = cent_ref.shape[0]
    per = LANES // capacity
    spans = col_count // per
    width = 2 * PAIRS * cb_hbm.shape[1]
    steps = v_ref.shape[1] // width
    last = count - per
    cuts = (0, steps - steps // 3, steps)

    top = col_count // 2
    quarter = col_count // 4
    zone = lax.div(col, quarter)
    inner = zone * (3 - zone) > 0
    outer = zone * (3 - zone) == 0
    mirror = xor(col, top + quarter, col_count)
    kin = row_count * top

    def same_slot(i):
        t = lax.rem(i, top)
        return lax.div(i, top) * col_count + t + lax.div(t, quarter) * top

    def cross_slot(i):
        return lax.div(i, top) * col_count + quarter + lax.rem(i, top)

    def place(slot):
        return xor(row, lax.div(slot, col_count), row_count), xor(col, lax.rem(slot, col_count), col_count)

    def piece(j):
        return book_ref.at[pl.ds(j * sub_local, sub_local)]

    def block(ref, owner):
        return ref.at[pl.ds(pl.multiple_of(owner * capacity, capacity), capacity)]

    cent_copy = pltpu.make_async_copy(cent_hbm, cent_ref, local_sem.at[0])
    book_copy = pltpu.make_async_copy(cb_hbm, piece(col), local_sem.at[1])
    v_copy = pltpu.make_async_copy(v_hbm, v_ref, local_sem.at[2])
    codes_copy = pltpu.make_async_copy(codes_hbm, codes_ref, local_sem.at[3])
    ids_local = pltpu.make_async_copy(ids_hbm, ids_ref, local_sem.at[5])
    fill_copy = pltpu.make_async_copy(fill_hbm, fill_ref, local_sem.at[6])
    ids_local.start()

    barrier = pltpu.get_barrier_semaphore()


    def signal(sem, slot):
        r, c = place(slot)
        pl.semaphore_signal(sem, inc=1, device_id=(r, c), device_id_type=pl.DeviceIdType.MESH)

    def greet_same(i, carry):
        signal(barrier, same_slot(i))
        return carry

    def greet_cross(i, carry):
        signal(barrier, cross_slot(i))
        return carry

    def tell_cross(i, carry):
        signal(ready, cross_slot(i))
        return carry

    def shift_ids():
        ids_local.wait()
        for p in range(per):
            ids = ids_ref[...]
            ids_own[p] = ids if p == 0 else pltpu.roll(ids, LANES - p * capacity, 1)

    lax.fori_loop(1, kin, greet_same, 0)

    @pl.when(inner)
    def _():
        lax.fori_loop(0, kin, greet_cross, 0)

    book_copy.start()
    cent_copy.start()
    fill_copy.start()
    shift_ids()
    v_copy.start()
    codes_copy.start()

    @pl.when(inner)
    def _():
        pl.semaphore_wait(barrier, kin - 1)

    @pl.when(outer)
    def _():
        pl.semaphore_wait(barrier, count - 1)
        lax.fori_loop(0, kin, tell_cross, 0)

    def ids_of(owner):
        return ids_own.at[lax.rem(owner, per), pl.ds(lax.div(owner, per), 1)]

    def ids_copy(slot):
        r, c = place(slot)
        return pltpu.make_async_remote_copy(
            src_ref=ids_of(r * col_count + c), dst_ref=ids_sm.at[pl.ds(me, 1)],
            send_sem=ids_send.at[slot], recv_sem=ids_recv.at[slot],
            device_id=(r, c), device_id_type=pl.DeviceIdType.MESH)

    def ids_arrived(slot):
        r, c = place(slot)
        return pltpu.make_async_remote_copy(
            src_ref=ids_of(me), dst_ref=ids_sm.at[pl.ds(r * col_count + c, 1)],
            send_sem=ids_send.at[slot], recv_sem=ids_recv.at[slot],
            device_id=(r, c), device_id_type=pl.DeviceIdType.MESH)

    def ids_same(i, carry):
        ids_copy(same_slot(kin - 1 - i)).start()
        return carry

    def ids_cross(i, carry):
        ids_copy(cross_slot(i)).start()
        return carry

    lax.fori_loop(0, kin - 1, ids_same, 0)

    @pl.when(outer)
    def _():
        lax.fori_loop(0, kin, ids_cross, 0)

    own_ids = pltpu.make_async_copy(
        ids_of(me), ids_sm.at[pl.ds(me, 1)], local_sem.at[4])
    own_ids.start()

    side = lax.rem(row, 2)
    peer = row + 1 - 2 * side

    def book_copy_to(source, target, sem):
        return pltpu.make_async_remote_copy(
            src_ref=piece(source), dst_ref=piece(source), send_sem=sem, recv_sem=book_recv.at[source],
            device_id=(row, target), device_id_type=pl.DeviceIdType.MESH)

    def peer_copy(k):
        j = 2 * k + side
        return pltpu.make_async_remote_copy(
            src_ref=piece(j), dst_ref=piece(j), send_sem=second_send.at[k], recv_sem=book_recv.at[j],
            device_id=(peer, col), device_id_type=pl.DeviceIdType.MESH)

    def arrived(j):
        return book_copy_to(j, mirror, first_send.at[0])

    def spread(source, sems, begin, end):
        return [book_copy_to(source, xor(col, b, col_count), sems.at[b]) for b in range(begin, end)]

    spreads = lax.rem(col, 2) == side
    book_copy.wait()

    @pl.when(spreads)
    def _():
        for copy in [book_copy_to(col, mirror, first_send.at[0])] + spread(col, first_send, 1, quarter):
            copy.start()

        @pl.when(outer)
        def _():
            for copy in spread(col, first_send, quarter, top):
                copy.start()

    def gather(owner, out_ref):
        out = block(out_ref, owner)
        for j in range(capacity):
            at = jnp.bitwise_and(ids_sm[owner, j], lists - 1)
            out[pl.ds(j, 1), :] = cent_ref[pl.ds(at, 1), :]

    def rows_copy(slot):
        r, c = place(slot)
        return pltpu.make_async_remote_copy(
            src_ref=block(wanted_ref, r * col_count + c), dst_ref=block(got_ref, me),
            send_sem=rows_send.at[slot], recv_sem=rows_recv.at[slot],
            device_id=(r, c), device_id_type=pl.DeviceIdType.MESH)

    def rows_arrived(slot):
        r, c = place(slot)
        return pltpu.make_async_remote_copy(
            src_ref=block(wanted_ref, me), dst_ref=block(got_ref, r * col_count + c),
            send_sem=rows_send.at[slot], recv_sem=rows_recv.at[slot],
            device_id=(r, c), device_id_type=pl.DeviceIdType.MESH)

    def last_part(f):
        return pl.ds(cuts[f] * width, (cuts[f + 1] - cuts[f]) * width)

    def last_copy(j, f):
        r, c = place(last + j)
        return pltpu.make_async_remote_copy(
            src_ref=block(wanted_ref, r * col_count + c).at[:, last_part(f)],
            dst_ref=block(got_ref, me).at[:, last_part(f)],
            send_sem=last_send.at[f, j], recv_sem=last_recv.at[f, j],
            device_id=(r, c), device_id_type=pl.DeviceIdType.MESH)

    def last_arrived(j, f):
        r, c = place(last + j)
        return pltpu.make_async_remote_copy(
            src_ref=block(wanted_ref, me).at[:, last_part(f)],
            dst_ref=block(got_ref, r * col_count + c).at[:, last_part(f)],
            send_sem=last_send.at[f, j], recv_sem=last_recv.at[f, j],
            device_id=(r, c), device_id_type=pl.DeviceIdType.MESH)

    def serve(first, end, before=None):
        def one(slot, carry):
            r, c = place(slot)
            ids_arrived(slot).wait_recv()
            gather(r * col_count + c, wanted_ref)

            @pl.when(slot > first)
            def _():
                @pl.when(slot <= last)
                def _():
                    rows_copy(slot - 1).start()

            if before is not None:
                @pl.when(slot == first)
                def _():
                    rows_copy(before).start()

            return carry

        lax.fori_loop(first, end, one, 0)
        return end - 1

    def forward():
        arrived(mirror).wait_recv()
        for copy in spread(mirror, mirror_send, 1, top):
            copy.start()

    @pl.when(outer)
    def _():
        @pl.when(spreads)
        def _():
            forward()

    cent_copy.wait()
    pending = serve(top + quarter, col_count)
    own_ids.wait()
    gather(me, got_ref)
    rows_copy(pending).start()

    @pl.when(inner)
    def _():
        pl.semaphore_wait(ready, kin)
        lax.fori_loop(0, kin, ids_cross, 0)

        @pl.when(spreads)
        def _():
            for copy in spread(col, first_send, quarter, top):
                copy.start()
            forward()

    pending = serve(1, quarter)
    for a in range(1, row_count // 2):
        pending = serve(a * col_count + top + quarter, (a + 1) * col_count, pending)
        pending = serve(a * col_count, a * col_count + quarter, pending)
    v_copy.wait()
    codes_copy.wait()
    rows_copy(pending).start()

    def pass_on(k, carry):
        j = 2 * k + side

        @pl.when((j - col) * (j - mirror) != 0)
        def _():
            arrived(j).wait_recv()

        @pl.when(j != col)
        def _():
            peer_copy(k).start()

        return carry

    lax.fori_loop(0, top, pass_on, 0)

    pending = None
    for a in range(row_count // 2):
        pending = serve(a * col_count + quarter, a * col_count + top + quarter, pending)
    serve((row_count // 2) * col_count, count, pending)

    def send_last(f):
        def one(j, carry):
            last_copy(j, f).start()
            return carry

        lax.fori_loop(0, per, one, 0)

    send_last(0)
    send_last(1)

    def from_peer(k, carry):
        j = 2 * k + 1 - side

        @pl.when(j != col)
        def _():
            arrived(j).wait_recv()

        return carry

    lax.fori_loop(0, top, from_peer, 0)
    build_table(book_ref, w_ref)

    lane = lax.broadcasted_iota(jnp.int32, (1, LANES), 1)
    sub_width = book_ref.shape[1]

    def group_at(g):
        a = lax.div(g, 2 * spans) * 2 + lax.rem(g, 2)
        h = lax.rem(lax.div(g, 2), spans)
        first = xor(row, a, row_count) * col_count + xor(lax.div(col, per), h, spans) * per
        return a * col_count + h * per, first, pl.multiple_of(first * capacity, LANES)

    def finish(carry, first, base):
        coded, best = score_end(carry)
        bound = jnp.zeros((1, LANES), jnp.int32)
        for j in range(per):
            bound = jnp.where(lane >= j * capacity, fill_ref[0, first + j] + j * capacity, bound)
        out_ref[0:1, pl.ds(base, LANES)] = coded
        out_ref[1:2, pl.ds(base, LANES)] = best
        out_ref[2:3, pl.ds(base, LANES)] = jnp.where(lane < bound, 1.0, 0.0)

    def out_copy(g):
        part = pl.ds(group_at(g)[2], LANES)
        return pltpu.make_async_copy(out_ref.at[:, part], out_hbm.at[:, part], out_sem.at[g])

    def out_wait(g, carry):
        out_copy(g).wait()
        return carry

    def group_step(g, carry):
        slot, first, base = group_at(g)

        def settle(j, inner):
            @pl.when(slot + j > 0)
            def _():
                rows_arrived(slot + j).wait_recv()

            return inner

        lax.fori_loop(0, per, settle, 0)
        rt_ref[...] = (v_ref[pl.ds(base, LANES), :] - got_ref[pl.ds(base, LANES), :]).T

        def step(f, inner):
            return score_step(f, inner, rt_ref, codes_ref, base, book_ref, w_ref)

        finish(lax.fori_loop(0, steps, step, score_start(sub_width)), first, base)

        @pl.when(g > 0)
        def _():
            out_copy(g - 1).start()

        return carry

    fill_copy.wait()
    lax.fori_loop(0, row_count * spans - 1, group_step, 0)

    def sent(src, sem):
        return pltpu.make_async_remote_copy(
            src_ref=src, dst_ref=src, send_sem=sem, recv_sem=ids_recv.at[0],
            device_id=(row, mirror), device_id_type=pl.DeviceIdType.MESH)

    def drain_ids(slot, carry):
        sent(ids_own.at[0, pl.ds(0, 1)], ids_send.at[slot]).wait_send()
        return carry

    def drain_rows(slot, carry):
        sent(block(wanted_ref, 0), rows_send.at[slot]).wait_send()
        return carry

    def drain_last(j, carry):
        for f in range(2):
            sent(block(wanted_ref, 0).at[:, last_part(f)], last_send.at[f, j]).wait_send()
        return carry

    lax.fori_loop(1, count, drain_ids, 0)
    lax.fori_loop(1, (row_count // 2) * col_count, drain_rows, 0)

    final = row_count * spans - 1
    out_copy(final - 1).start()
    _, first, base = group_at(final)

    carry = score_start(sub_width)
    for f in range(2):
        for j in range(per):
            last_arrived(j, f).wait_recv()
        part = last_part(f)
        rt_ref[part, :] = (v_ref[pl.ds(base, LANES), part] - got_ref[pl.ds(base, LANES), part]).T

        def last_step(g, inside):
            return score_step(g, inside, rt_ref, codes_ref, base, book_ref, w_ref)

        carry = lax.fori_loop(cuts[f], cuts[f + 1], last_step, carry)
    finish(carry, first, base)

    @pl.when(spreads)
    def _():
        book_copy_to(col, mirror, first_send.at[0]).wait_send()
        for copy in spread(col, first_send, 1, top) + spread(mirror, mirror_send, 1, top):
            copy.wait_send()

    def drain_peer(k, carry):
        @pl.when(2 * k + side != col)
        def _():
            peer_copy(k).wait_send()

        return carry

    lax.fori_loop(0, top, drain_peer, 0)

    lax.fori_loop((row_count // 2) * col_count, last, drain_rows, 0)
    out_copy(final).start()
    lax.fori_loop(0, per, drain_last, 0)
    lax.fori_loop(0, final + 1, out_wait, 0)


def local(vectors, list_ids, pq_codes, fill_counts, centroids, codebook):
    row_count = lax.axis_size("row")
    col_count = lax.axis_size("col")
    count = row_count * col_count
    slot_count, feature_width = vectors.shape
    sub_total = pq_codes.shape[1]
    sub_width, code_count = codebook.shape[1:]
    per = LANES * count // slot_count
    hbm = pl.BlockSpec(memory_space=pl.ANY)
    coded, best, live = pl.pallas_call(
        functools.partial(exchange_kernel, row_count, col_count),
        out_shape=jax.ShapeDtypeStruct((3, slot_count), F32),
        in_specs=[hbm] * 6,
        out_specs=hbm,
        scratch_shapes=[
            pltpu.VMEM((slot_count, feature_width), F32),
            pltpu.VMEM((slot_count, feature_width), F32),
            pltpu.VMEM((slot_count, feature_width), F32),
            pltpu.VMEM(centroids.shape, F32),
            pltpu.VMEM((sub_total, slot_count), jnp.int32),
            pltpu.VMEM((sub_total, sub_width, code_count), F32),
            pltpu.VMEM((sub_total // 2, code_count, 2 * DEPTH), BF16),
            pltpu.VMEM((feature_width, LANES), F32),
            pltpu.VMEM((3, slot_count), F32),
            pltpu.VMEM((slot_count // LANES, LANES), jnp.int32),
            pltpu.VMEM((per, slot_count // LANES, LANES), jnp.int32),
            pltpu.SMEM(fill_counts.shape, jnp.int32),
            pltpu.SMEM((count, LANES), jnp.int32),
            pltpu.SemaphoreType.DMA((7,)),
            pltpu.SemaphoreType.REGULAR,
            pltpu.SemaphoreType.DMA((count,)),
            pltpu.SemaphoreType.DMA((count,)),
            pltpu.SemaphoreType.DMA((col_count // 2,)),
            pltpu.SemaphoreType.DMA((col_count // 2,)),
            pltpu.SemaphoreType.DMA((col_count // 2,)),
            pltpu.SemaphoreType.DMA((col_count,)),
            pltpu.SemaphoreType.DMA((count,)),
            pltpu.SemaphoreType.DMA((count,)),
            pltpu.SemaphoreType.DMA((2, per)),
            pltpu.SemaphoreType.DMA((2, per)),
            pltpu.SemaphoreType.DMA((slot_count // LANES,)),
        ],
        compiler_params=pltpu.CompilerParams(
            collective_id=0, has_side_effects=True, vmem_limit_bytes=56 * 2**20),
        name="exchange_score",
    )(codebook, vectors, pq_codes.T, centroids, list_ids.reshape(slot_count // LANES, LANES), fill_counts)
    return jnp.where(live > 0.0, coded, 0.0), jnp.where(live > 0.0, best, 0.0)


def solution(mesh):
    in_specs = (
        P(("row", "col"), None),
        P(("row", "col")),
        P(("row", "col"), None),
        P(("row", "col"), None),
        P(("row", "col"), None),
        P("col", None, None),
    )
    out_specs = (P(("row", "col")), P(("row", "col")))
    return jax.shard_map(local, mesh=mesh, in_specs=in_specs, out_specs=out_specs, check_vma=False)
```
